32 devices in a mesh: dp: 4 (over y, z), tp: 8 (over x, core).
Axes of the slice: x: 4, y: 2, z: 2, core: 2. Of those that a mesh axis runs over, the one named last changes fastest.
The devices are a block of a 4x4x8 slice.
Arguments:
- x_in: bfloat16 [8, 2048, 1024], P('dp', 'tp'), parts along dimension 0
- x_mid: bfloat16 [8, 2048, 1024], P('dp', 'tp'), parts along dimension 0
- d_out: bfloat16 [8, 2048, 1024], P('dp', 'tp'), parts along dimension 0
- q_saved: bfloat16 [8, 2048, 16, 64], P('dp', None, 'tp'), parts along dimension 0
- k_saved: bfloat16 [8, 2048, 16, 64], P('dp', None, 'tp'), parts along dimension 0
- v_saved: bfloat16 [8, 2048, 16, 64], P('dp', None, 'tp'), parts along dimension 0
- z_saved: bfloat16 [8, 2048, 4096], P('dp', None, 'tp'), parts along dimension 0
- ln1_gain: float32 [1024], replicated
- ln1_bias: float32 [1024], replicated
- ln2_gain: float32 [1024], replicated
- ln2_bias: float32 [1024], replicated
- w_qkv: bfloat16 [3, 1024, 16, 64], P(None, None, 'tp')
- w_proj: bfloat16 [16, 64, 1024], P('tp')
- w_fc1: bfloat16 [1024, 4096], P(None, 'tp')
- w_fc2: bfloat16 [4096, 1024], P('tp')
Outputs:
- output 1: bfloat16 [8, 2048, 1024], P('dp', 'tp'), parts along dimension 0
- output 2: float32 [12, 1024, 16, 64], P('dp', None, 'tp'), parts along dimension 0
- output 3: float32 [12, 16, 64], P('dp', 'tp'), parts along dimension 0
- output 4: float32 [64, 64, 1024], P(('dp', 'tp')), parts along dimension 0
- output 5: float32 [4096, 4096], P('dp', 'tp'), parts along dimension 0
- output 6: float32 [16384], P(('dp', 'tp')), parts along dimension 0
- output 7: float32 [16384, 1024], P(('dp', 'tp')), parts along dimension 0
- output 8: float32 [24, 1024], P('dp'), parts along dimension 0
There are 4 independent parts. The reference program is written for one: setup_inputs(seed, part) draws one part's arguments, and reference() takes and returns one part's arrays. A program takes and returns all parts, laid end to end along the dimension named above; an argument that names none is the same for every part.
All inputs are finite; a program needn't handle non-finite values.
Results may differ from the reference program's by a relative error of at most 0.0114087.
Values are sent between devices in bfloat16 or wider.
A program may use at most 768 MiB of HBM per device.

```python
import jax
import jax.numpy as jnp
from jax import lax

BATCH_SEQS = 2
SEQ_LEN = 2048
D_MODEL = 1024
N_HEADS = 16
HEAD_DIM = 64
FF_DIM = 4096
LN_EPS = 1e-5
GELU_COEF = 0.044715
GELU_SCALE = 0.7978845608028654


def draw_normal(key, shape, scale):
    return (scale * jax.random.normal(key, shape, jnp.float32)).astype(jnp.bfloat16)


def setup_inputs(seed: int = 0, part: int = 0) -> dict:
    part_keys = jax.random.split(jax.random.fold_in(jax.random.key(seed), part), 7)
    shared_keys = jax.random.split(jax.random.key(seed + 1), 8)
    tok_shape = (BATCH_SEQS, SEQ_LEN, D_MODEL)
    head_shape = (BATCH_SEQS, SEQ_LEN, N_HEADS, HEAD_DIM)
    return {
        'x_in': draw_normal(part_keys[0], tok_shape, 1.0),
        'x_mid': draw_normal(part_keys[1], tok_shape, 1.0),
        'd_out': draw_normal(part_keys[2], tok_shape, 1.0),
        'q_saved': draw_normal(part_keys[3], head_shape, 1.0),
        'k_saved': draw_normal(part_keys[4], head_shape, 1.0),
        'v_saved': draw_normal(part_keys[5], head_shape, 1.0),
        'z_saved': draw_normal(part_keys[6], (BATCH_SEQS, SEQ_LEN, FF_DIM), 1.5),
        'ln1_gain': jax.random.uniform(shared_keys[0], (D_MODEL,), jnp.float32, 0.5, 1.5),
        'ln1_bias': 0.5 * jax.random.normal(shared_keys[1], (D_MODEL,), jnp.float32),
        'ln2_gain': jax.random.uniform(shared_keys[2], (D_MODEL,), jnp.float32, 0.5, 1.5),
        'ln2_bias': 0.5 * jax.random.normal(shared_keys[3], (D_MODEL,), jnp.float32),
        'w_qkv': draw_normal(shared_keys[4], (3, D_MODEL, N_HEADS, HEAD_DIM), D_MODEL ** -0.5),
        'w_proj': draw_normal(shared_keys[5], (N_HEADS, HEAD_DIM, D_MODEL), D_MODEL ** -0.5),
        'w_fc1': draw_normal(shared_keys[6], (D_MODEL, FF_DIM), D_MODEL ** -0.5),
        'w_fc2': draw_normal(shared_keys[7], (FF_DIM, D_MODEL), FF_DIM ** -0.5),
    }


def layer_norm_fwd(token_rows, norm_gain, norm_bias):
    rows_f32 = token_rows.astype(jnp.float32)
    centered = rows_f32 - jnp.mean(rows_f32, axis=-1, keepdims=True)
    inv_std = lax.rsqrt(jnp.mean(centered * centered, axis=-1, keepdims=True) + LN_EPS)
    x_hat = centered * inv_std
    return x_hat, inv_std, (x_hat * norm_gain + norm_bias).astype(jnp.bfloat16)


def layer_norm_bwd(grad_norm, x_hat, inv_std, norm_gain):
    grad_hat = grad_norm * norm_gain
    centered_grad = grad_hat - jnp.mean(grad_hat, axis=-1, keepdims=True)
    return inv_std * (centered_grad - x_hat * jnp.mean(grad_hat * x_hat, axis=-1, keepdims=True))


def gelu_parts(pre_act):
    tanh_val = jnp.tanh(GELU_SCALE * (pre_act + GELU_COEF * pre_act * pre_act * pre_act))
    act_value = 0.5 * pre_act * (1.0 + tanh_val)
    act_slope = 0.5 * (1.0 + tanh_val) + 0.5 * pre_act * (1.0 - tanh_val * tanh_val) * GELU_SCALE * (1.0 + 3.0 * GELU_COEF * pre_act * pre_act)
    return act_value, act_slope


def head_attention_grads(operands):
    q_head, k_head, v_head, dctx_head = operands
    score_scale = HEAD_DIM ** -0.5
    q_wide = q_head.astype(jnp.float32)
    k_wide = k_head.astype(jnp.float32)
    v_wide = v_head.astype(jnp.float32)
    dctx_wide = dctx_head.astype(jnp.float32)
    scores = jnp.einsum('bqe,bke->bqk', q_wide, k_wide) * score_scale
    row_ids = lax.broadcasted_iota(jnp.int32, (SEQ_LEN, SEQ_LEN), 0)
    col_ids = lax.broadcasted_iota(jnp.int32, (SEQ_LEN, SEQ_LEN), 1)
    scores = jnp.where(row_ids >= col_ids, scores, -1e30)
    attn_probs = jax.nn.softmax(scores, axis=-1)
    probs_low = attn_probs.astype(jnp.bfloat16).astype(jnp.float32)
    context = jnp.einsum('bqk,bke->bqe', probs_low, v_wide).astype(jnp.bfloat16)
    grad_probs = jnp.einsum('bqe,bke->bqk', dctx_wide, v_wide)
    grad_scores = attn_probs * (grad_probs - jnp.sum(grad_probs * attn_probs, axis=-1, keepdims=True)) * score_scale
    scores_low = grad_scores.astype(jnp.bfloat16).astype(jnp.float32)
    grad_q = jnp.einsum('bqk,bke->bqe', scores_low, k_wide).astype(jnp.bfloat16)
    grad_k = jnp.einsum('bqk,bqe->bke', scores_low, q_wide).astype(jnp.bfloat16)
    grad_v = jnp.einsum('bqk,bqe->bke', probs_low, dctx_wide).astype(jnp.bfloat16)
    return context, grad_q, grad_k, grad_v


def reference(x_in, x_mid, d_out, q_saved, k_saved, v_saved, z_saved, ln1_gain, ln1_bias, ln2_gain, ln2_bias, w_qkv, w_proj, w_fc1, w_fc2):
    n_tok = BATCH_SEQS * SEQ_LEN
    norm2_hat, norm2_rstd, h2_norm = layer_norm_fwd(x_mid, ln2_gain, ln2_bias)
    act_value, act_slope = gelu_parts(z_saved.astype(jnp.float32))
    dout_rows = d_out.reshape(n_tok, D_MODEL)
    grad_wfc2 = jnp.dot(act_value.astype(jnp.bfloat16).reshape(n_tok, FF_DIM).T, dout_rows, preferred_element_type=jnp.float32)
    grad_act = jnp.dot(dout_rows, w_fc2.T, preferred_element_type=jnp.float32)
    grad_pre = (grad_act * act_slope.reshape(n_tok, FF_DIM)).astype(jnp.bfloat16)
    grad_wfc1 = jnp.dot(h2_norm.reshape(n_tok, D_MODEL).T, grad_pre, preferred_element_type=jnp.float32)
    grad_bfc1 = jnp.sum(grad_pre.astype(jnp.float32), axis=0)
    grad_h2 = jnp.dot(grad_pre, w_fc1.T, preferred_element_type=jnp.float32).reshape(BATCH_SEQS, SEQ_LEN, D_MODEL)
    grad_mid = (d_out.astype(jnp.float32) + layer_norm_bwd(grad_h2, norm2_hat, norm2_rstd, ln2_gain)).astype(jnp.bfloat16)
    mid_rows = grad_mid.reshape(n_tok, D_MODEL)
    grad_ctx = jnp.dot(mid_rows, w_proj.reshape(D_MODEL, D_MODEL).T, preferred_element_type=jnp.float32).astype(jnp.bfloat16)
    grad_ctx = grad_ctx.reshape(BATCH_SEQS, SEQ_LEN, N_HEADS, HEAD_DIM)
    context, grad_q, grad_k, grad_v = lax.map(head_attention_grads, (jnp.moveaxis(q_saved, 2, 0), jnp.moveaxis(k_saved, 2, 0), jnp.moveaxis(v_saved, 2, 0), jnp.moveaxis(grad_ctx, 2, 0)))
    context_rows = jnp.moveaxis(context, 0, 2).reshape(n_tok, D_MODEL)
    grad_wproj = jnp.dot(context_rows.T, mid_rows, preferred_element_type=jnp.float32).reshape(N_HEADS, HEAD_DIM, D_MODEL)
    norm1_hat, norm1_rstd, h1_norm = layer_norm_fwd(x_in, ln1_gain, ln1_bias)
    qkv_rows = jnp.moveaxis(jnp.stack([grad_q, grad_k, grad_v]), 1, 3).reshape(3, n_tok, D_MODEL).astype(jnp.float32)
    grad_wqkv = jnp.einsum('td,ite->ide', h1_norm.reshape(n_tok, D_MODEL).astype(jnp.float32), qkv_rows).reshape(3, D_MODEL, N_HEADS, HEAD_DIM)
    grad_bqkv = jnp.sum(qkv_rows, axis=1).reshape(3, N_HEADS, HEAD_DIM)
    grad_h1 = jnp.einsum('ite,ide->td', qkv_rows, w_qkv.reshape(3, D_MODEL, D_MODEL).astype(jnp.float32)).reshape(BATCH_SEQS, SEQ_LEN, D_MODEL)
    grad_x = (grad_mid.astype(jnp.float32) + layer_norm_bwd(grad_h1, norm1_hat, norm1_rstd, ln1_gain)).astype(jnp.bfloat16)
    grad_vecs = jnp.stack([
        jnp.sum(grad_h1 * norm1_hat, axis=(0, 1)),
        jnp.sum(grad_h1, axis=(0, 1)),
        jnp.sum(grad_h2 * norm2_hat, axis=(0, 1)),
        jnp.sum(grad_h2, axis=(0, 1)),
        jnp.sum(grad_mid.astype(jnp.float32), axis=(0, 1)),
        jnp.sum(d_out.astype(jnp.float32), axis=(0, 1)),
    ])
    return grad_x, grad_wqkv, grad_bqkv, grad_wproj, grad_wfc1, grad_bfc1, grad_wfc2, grad_vecs
```

```python
import functools

import jax
import jax.numpy as jnp
from jax import lax
from jax.experimental import pallas as pl
from jax.experimental.pallas import tpu as pltpu
from jax.sharding import PartitionSpec as P

LN_EPS = 1e-5
GELU_COEF = 0.044715
GELU_SCALE = 0.7978845608028654
LOG2E = 1.4426950408889634
MESH = pl.DeviceIdType.MESH
F32 = jnp.float32
BF16 = jnp.bfloat16
VMEM_LIMIT = 67043328

NN = (((1,), (0,)), ((), ()))
NT = (((1,), (1,)), ((), ()))
TN = (((0,), (0,)), ((), ()))

CORES = 2
BATCH = range(2)
HEADS = range(2)
RING = R_RIGHT, R_FAR, R_LEFT = 1, 2, 3
SLOT_P, SLOT_R, SLOT_F, SLOT_L, SLOT_END = 1, 2, 4, 6, 8
PARTNER, RIGHT, LEFT, FWD_R, FWD_L = range(5)
NEAR_R, NEAR_L, FAR_R, FAR_L, LAST_R, LAST_L = range(4, 10)
SUB = 8
LANES = 128
TK = 512
NC = 256
STEP = 64


def mm(a, b, dims):
    return lax.dot_general(a, b, dims, preferred_element_type=F32)


def loop(count, body):
    def run(i, carry):
        body(i)
        return carry
    lax.fori_loop(0, count, run, 0)


def fold8(v):
    return jnp.sum(v.reshape(v.shape[0] // SUB, SUB, v.shape[1]), axis=0)


def turn(v):
    return jnp.transpose(v.astype(F32)).astype(BF16)


def span(i, size):
    return pl.ds(pl.multiple_of(i * size, size), size)


def columns(width):
    return [pl.ds(n * NC, NC) for n in range(width // NC)]


def clear(*refs):
    for ref in refs:
        ref[...] = jnp.zeros_like(ref)


def ln_stats(rows):
    centered = rows - jnp.mean(rows, axis=-1, keepdims=True)
    inv_std = lax.rsqrt(jnp.mean(centered * centered, axis=-1, keepdims=True) + LN_EPS)
    return centered * inv_std, inv_std


def ln_bwd(grad, x_hat, inv_std, gain):
    grad_hat = grad * gain
    centered = grad_hat - jnp.mean(grad_hat, axis=-1, keepdims=True)
    return inv_std * (centered - x_hat * jnp.mean(grad_hat * x_hat, axis=-1, keepdims=True))


def normalize(src, dst, gain, bias):
    per = src.shape[1] // STEP

    def body(i):
        b, rs = i // per, span(lax.rem(i, per), STEP)
        x_hat, _ = ln_stats(src[b, rs].astype(F32))
        dst[0, b, rs] = (x_hat * gain[...] + bias[...]).astype(BF16)

    loop(len(BATCH) * per, body)


def start_copies(pairs, sems):
    copies = [pltpu.make_async_copy(s, d, sems.at[i]) for i, (s, d) in enumerate(pairs)]
    for copy in copies:
        copy.start()
    return copies


class Place:
    def __init__(self, n_tp):
        self.chips = n_tp // CORES
        me = lax.axis_index('tp')
        self.x = me // CORES
        self.c = lax.rem(me, CORES)
        self.partner = self.block(0, 1)
        self.right, self.far, self.left = [self.block(r, 0) for r in RING]

    def block(self, r, p):
        return lax.rem(self.x + r, self.chips) * CORES + lax.rem(self.c + p, CORES)

    def enter(self, peers):
        barrier = pltpu.get_barrier_semaphore()
        for peer in peers:
            pl.semaphore_signal(barrier, inc=1, device_id={'tp': peer}, device_id_type=MESH)
        pl.semaphore_wait(barrier, len(peers))


def remote(src, dst, ssem, rsem, peer):
    return pltpu.make_async_remote_copy(src_ref=src, dst_ref=dst, send_sem=ssem, recv_sem=rsem,
                                        device_id={'tp': peer}, device_id_type=MESH)


class Gather:
    def __init__(self, place, own, buf, ssem, rsem):
        self.place, self.own, self.buf, self.ssem, self.rsem = place, own, buf, ssem, rsem
        half = buf.shape[-2] // 2
        self.lo, self.hi = pl.ds(0, half), pl.ds(half, half)

    def _own(self, kind, slot, b, peer):
        return remote(self.own.at[b], self.buf.at[slot, b], self.ssem.at[kind, b], self.rsem.at[slot, b], peer)

    def to_partner(self, b):
        return self._own(PARTNER, SLOT_P, b, self.place.partner)

    def to_right(self, b):
        return self._own(RIGHT, SLOT_L, b, self.place.right)

    def to_left(self, b):
        return self._own(LEFT, SLOT_R, b, self.place.left)

    def fwd_right(self, b):
        return remote(self.buf.at[SLOT_L, b, self.lo], self.buf.at[SLOT_F, b, self.lo],
                      self.ssem.at[FWD_R, b], self.rsem.at[SLOT_F, b], self.place.right)

    def fwd_left(self, b):
        return remote(self.buf.at[SLOT_R, b, self.hi], self.buf.at[SLOT_F, b, self.hi],
                      self.ssem.at[FWD_L, b], self.rsem.at[SLOT_END, b], self.place.left)

    def share(self, r, b):
        slot = CORES * r
        return remote(self.buf.at[slot, b], self.buf.at[slot + 1, b], self.ssem.at[FWD_L + r, b], self.rsem.at[slot + 1, b],
                      self.place.partner)

    def start_own(self, b):
        self.to_right(b).start()
        self.to_left(b).start()
        self.to_partner(b).start()

    def relay(self, b):
        self.to_right(b).wait_recv()
        self.fwd_right(b).start()
        self.to_left(b).wait_recv()
        self.fwd_left(b).start()
        self.share(R_LEFT, b).start()
        self.share(R_RIGHT, b).start()

    def relay_far(self, b):
        self.fwd_right(b).wait_recv()
        self.fwd_left(b).wait_recv()
        self.share(R_FAR, b).start()

    def wait_shared(self, r, b):
        self.share(r, b).wait_recv()

    def wait_partner(self, b):
        self.to_partner(b).wait_recv()

    def finish(self):
        for b in BATCH:
            for copy in (self.to_partner(b), self.to_right(b), self.to_left(b), self.fwd_right(b), self.fwd_left(b),
                         *(self.share(r, b) for r in RING)):
                copy.wait_send()


class Scatter:
    def __init__(self, place, p_out, p_in, sums, fin, transit, ssem, rsem):
        self.place = place
        self.p_out, self.p_in, self.sums, self.fin, self.transit = p_out, p_in, sums, fin, transit
        self.ssem, self.rsem = ssem, rsem
        half = sums.shape[-2] // 2
        self.lo, self.hi = pl.ds(0, half), pl.ds(half, half)

    def to_partner(self, r, b):
        return remote(self.p_out.at[r, b], self.p_in.at[r, b], self.ssem.at[r, b], self.rsem.at[r, b], self.place.partner)

    def _hop(self, kind, src, dst, b, peer):
        return remote(src, dst, self.ssem.at[kind, b], self.rsem.at[kind, b], peer)

    def near_right(self, b):
        return self._hop(NEAR_R, self.sums.at[0, b, self.hi], self.fin.at[0, b, self.hi], b, self.place.right)

    def near_left(self, b):
        return self._hop(NEAR_L, self.sums.at[2, b, self.lo], self.fin.at[1, b, self.lo], b, self.place.left)

    def far_right(self, b):
        return self._hop(FAR_R, self.sums.at[1, b, self.lo], self.transit.at[0, b], b, self.place.right)

    def far_left(self, b):
        return self._hop(FAR_L, self.sums.at[1, b, self.hi], self.transit.at[1, b], b, self.place.left)

    def last_right(self, b):
        return self._hop(LAST_R, self.sums.at[0, b, self.lo], self.fin.at[0, b, self.lo], b, self.place.right)

    def last_left(self, b):
        return self._hop(LAST_L, self.sums.at[2, b, self.hi], self.fin.at[1, b, self.hi], b, self.place.left)

    def send_near(self, b):
        self.near_right(b).start()
        self.near_left(b).start()

    def send_far(self, b):
        self.far_right(b).start()
        self.far_left(b).start()

    def send_last(self, b):
        for arrived, slot, lane, rows, onward in ((self.far_right, 0, 0, self.lo, self.last_right),
                                                  (self.far_left, 2, 1, self.hi, self.last_left)):
            arrived(b).wait_recv()
            self.sums[slot, b, rows] = (self.sums[slot, b, rows].astype(F32) + self.transit[lane, b].astype(F32)).astype(BF16)
            onward(b).start()

    def wait_final(self, b):
        for copy in (self.near_right, self.near_left, self.last_right, self.last_left):
            copy(b).wait_recv()

    def total(self, own, b, rs):
        return own[b, rs] + self.fin[0, b, rs].astype(F32) + self.fin[1, b, rs].astype(F32)

    def finish(self):
        for b in BATCH:
            for r in (0, *RING):
                self.to_partner(r, b).wait_send()
            for copy in (self.near_right, self.near_left, self.far_right, self.far_left, self.last_right, self.last_left):
                copy(b).wait_send()


def scatter_scratch(rows, width):
    def buf(*lead):
        return pltpu.VMEM((*lead, len(BATCH), rows, width), BF16)
    return [buf(4), buf(4), buf(3), buf(2), pltpu.VMEM((2, len(BATCH), rows // 2, width), BF16),
            pltpu.SemaphoreType.DMA((10, 2)), pltpu.SemaphoreType.DMA((10, 2))]


def gather_scratch(rows, width):
    return [pltpu.VMEM((SLOT_END, len(BATCH), rows, width), BF16),
            pltpu.SemaphoreType.DMA((SLOT_END, 2)), pltpu.SemaphoreType.DMA((SLOT_END + 1, 2))]


def first_head(shape):
    return lax.broadcasted_iota(jnp.int32, shape, 1) < shape[1] // len(HEADS)


def split_heads(v):
    first, zero = first_head(v.shape), jnp.zeros_like(v)
    return [jnp.where(first, v, zero), jnp.where(first, zero, v)]


def visible(blk, j, rows):
    row_id = blk * rows + lax.broadcasted_iota(jnp.int32, (rows, TK), 0)
    return row_id >= j * TK + lax.broadcasted_iota(jnp.int32, (rows, TK), 1)


def attn_fwd_block(b, blk, q_t, k_t, v_t, ctx_t, ctx, lse, s_buf, m_buf, scale):
    rows = ctx.shape[2]
    qs = span(blk, rows)
    last = blk // (TK // rows)
    q_h = split_heads(turn(q_t[b, :, qs]))

    def fold(f, v):
        parts = [v[:, i:i + LANES] for i in range(0, TK, LANES)]
        return functools.reduce(f, parts)

    def score(j, masked=False):
        kk = k_t[b, :, span(j, TK)]
        for h in HEADS:
            s = mm(q_h[h], kk, NN) * scale
            if masked:
                s = jnp.where(visible(blk, j, rows), s, -1e30)
            s_buf[h, :, span(j, TK)] = s
            top = fold(jnp.maximum, s)
            m_buf[h] = top if masked else jnp.maximum(m_buf[h], top)

    score(last, True)
    loop(last, score)
    m_col = [jnp.max(m_buf[h], axis=-1, keepdims=True) for h in HEADS]
    clear(m_buf)

    def total(j):
        for h in HEADS:
            m_buf[h] += fold(jnp.add, jnp.exp2(s_buf[h, :, span(j, TK)] - m_col[h]))

    loop(last + 1, total)
    l_col = [m_col[h] + jnp.log2(jnp.sum(m_buf[h], axis=-1, keepdims=True)) for h in HEADS]
    clear(m_buf)

    def weigh(j):
        vv = v_t[b, :, span(j, TK)]
        for h in HEADS:
            m_buf[h] += mm(jnp.exp2(s_buf[h, :, span(j, TK)] - l_col[h]).astype(BF16), vv, NT)

    loop(last + 1, weigh)
    first = first_head(m_buf.shape[1:])
    out = jnp.where(first, m_buf[0], m_buf[1])
    ctx[b, blk] = out
    lse[b, blk] = jnp.where(first, *l_col)
    ctx_t[b, :, qs] = turn(out)


def mlp_kernel(n_tp, scale, dy_hbm, xm_hbm, z_hbm, w1_hbm, w2_hbm, q_hbm, k_hbm, v_hbm, gain_ref, bias_ref,
               dx1_hbm, dw1_hbm, dw2_hbm, ctxt_hbm, ctx_hbm, lse_hbm, db1_ref, vec_ref,
               dyb, dy_ss, dy_rs, hb, h_ss, h_rs, p_out, p_in, sums, fin, transit, rs_ss, rs_rs,
               z, w1, w2, dw1, dw2, own, xm, db1, q_t, k_t, v_t, ctx_t, ctx, lse, s_buf, m_buf, lsem):
    place = Place(n_tp)
    rows, width = dy_hbm.shape[1:]
    units = w2.shape[0]
    blocks = ctx.shape[1]
    place.enter((place.partner, place.right, place.left))
    dyg = Gather(place, dy_hbm, dyb, dy_ss, dy_rs)
    hg = Gather(place, hb.at[0], hb, h_ss, h_rs)
    sc = Scatter(place, p_out, p_in, sums, fin, transit, rs_ss, rs_rs)
    for b in BATCH:
        dyg.start_own(b)
    loads = start_copies(((xm_hbm, xm), (dy_hbm, dyb.at[0]), (w2_hbm, w2), (z_hbm, z), (w1_hbm, w1),
                          (q_hbm, q_t), (k_hbm, k_t), (v_hbm, v_t)), lsem)
    clear(dw1, dw2, db1, vec_ref)
    loads[0].wait()
    normalize(xm, hb, gain_ref, bias_ref)
    for load in loads[1:]:
        load.wait()

    def attend(lo, count):
        def body(i):
            i = lo + i
            attn_fwd_block(i // blocks, lax.rem(i, blocks), q_t, k_t, v_t, ctx_t, ctx, lse, s_buf, m_buf, scale)
        loop(count, body)

    def pre_piece(r, p, b):
        dy, blk = dyb[CORES * r + p, b], place.block(r, p)
        for fs in columns(units):
            act = mm(dy, w2[fs, :], NT)
            zf = z[b, blk, :, fs].astype(F32)
            t = jnp.tanh(GELU_SCALE * (zf + GELU_COEF * zf * zf * zf))
            half_t = 0.5 * (1.0 + t)
            slope = half_t + 0.5 * zf * (1.0 - t * t) * GELU_SCALE * (1.0 + 3.0 * GELU_COEF * zf * zf)
            u = (zf * half_t).astype(BF16)
            dzv = (act * slope).astype(BF16)
            z[b, blk, :, fs] = dzv
            db1[:, fs] += fold8(dzv.astype(F32))
            dw2[fs, :] += mm(u, dy, TN)
        return z[b, blk]

    def pair(r, b, put):
        dz = pre_piece(r, 1, b)
        for ns in columns(width):
            p_out[r, b, :, ns] = mm(dz, w1[ns, :], NT).astype(BF16)
        sc.to_partner(r, b).start()
        dz = pre_piece(r, 0, b)
        sc.to_partner(r, b).wait_recv()
        for ns in columns(width):
            put(ns, mm(dz, w1[ns, :], NT) + p_in[r, b, :, ns].astype(F32))

    def pair_out(r, b):
        dyg.wait_shared(r, b)

        def put(ns, v):
            sums[r - 1, b, :, ns] = v.astype(BF16)
        pair(r, b, put)

    def own_body(b):
        dyg.wait_partner(b)

        def put(ns, v):
            own[b, :, ns] = v
        pair(0, b, put)

    def near_body(b):
        dyg.relay(b)
        loop(2, lambda i: pair_out(R_RIGHT + 2 * i, b))
        sc.send_near(b)
        attend(2 * b, 2)

    def far_body(b):
        dyg.relay_far(b)
        pair_out(R_FAR, b)
        sc.send_far(b)
        hg.start_own(b)

    def dw1_pair(r, b):
        def body(p):
            dw1[...] += mm(hb[CORES * r + p, b], z[b, place.block(r, p)], TN)
        loop(CORES, body)

    def dw1_own(b):
        hg.wait_partner(b)
        dw1_pair(0, b)

    def dw1_near(b):
        def body(i):
            r = R_RIGHT + 2 * i
            hg.wait_shared(r, b)
            dw1_pair(r, b)
        loop(2, body)

    def dw1_far(b):
        hg.relay_far(b)
        hg.wait_shared(R_FAR, b)
        dw1_pair(R_FAR, b)

    def back(b):
        sc.wait_final(b)

        def body(i):
            rs = span(i, STEP)
            grad = sc.total(own, b, rs)
            x_hat, inv_std = ln_stats(xm[b, rs].astype(F32))
            dyf = dyb[0, b, rs].astype(F32)
            dx1 = (dyf + ln_bwd(grad, x_hat, inv_std, gain_ref[...])).astype(BF16)
            xm[b, rs] = dx1
            for k, v in enumerate((grad * x_hat, grad, dx1.astype(F32), dyf)):
                vec_ref[k] += fold8(v)
        loop(rows // STEP, body)

    loop(2, own_body)
    loop(2, near_body)
    loop(2, far_body)
    rest = 2 * blocks - 4
    attend(4, rest)
    ctx_stores = start_copies(((ctx_t, ctxt_hbm), (ctx, ctx_hbm), (lse, lse_hbm)), lsem)
    loop(2, sc.send_last)
    hg.relay(0)
    loop(2, dw1_own)
    hg.relay(1)
    loop(2, dw1_near)
    loop(2, back)
    for store in ctx_stores:
        store.wait()
    stores = start_copies(((xm, dx1_hbm), (dw2, dw2_hbm)), lsem)
    db1_ref[...] = jnp.sum(db1[...], axis=0, keepdims=True)
    loop(2, dw1_far)
    for store in stores:
        store.wait()
    stores = start_copies(((dw1, dw1_hbm),), lsem)
    dyg.finish()
    hg.finish()
    sc.finish()
    stores[0].wait()


def mlp_backward(n_tp, scale, d_out, x_mid, z, w1, w2, q_t, k_t, v_t, gain, bias):
    batch, rows, width = d_out.shape
    units = w2.shape[0]
    seq = q_t.shape[2]
    blocks = seq // rows
    any_spec = pl.BlockSpec(memory_space=pl.ANY)
    vm = pl.BlockSpec(memory_space=pltpu.VMEM)
    heads_t = (batch, LANES, seq)
    per_row = (batch, blocks, rows, LANES)
    return pl.pallas_call(
        functools.partial(mlp_kernel, n_tp, scale),
        name='mlp_backward',
        out_shape=(jax.ShapeDtypeStruct((batch, rows, width), BF16), jax.ShapeDtypeStruct((width, units), F32),
                   jax.ShapeDtypeStruct((units, width), F32), jax.ShapeDtypeStruct(heads_t, BF16),
                   jax.ShapeDtypeStruct(per_row, F32), jax.ShapeDtypeStruct(per_row, F32),
                   jax.ShapeDtypeStruct((1, units), F32), jax.ShapeDtypeStruct((4, SUB, width), F32)),
        in_specs=[any_spec] * 8 + [vm] * 2,
        out_specs=(*[any_spec] * 6, vm, vm),
        scratch_shapes=gather_scratch(rows, width) + gather_scratch(rows, width) + scatter_scratch(rows, width) + [
            pltpu.VMEM((batch, blocks, rows, units), BF16),
            pltpu.VMEM((width, units), BF16), pltpu.VMEM((units, width), BF16),
            pltpu.VMEM((width, units), F32), pltpu.VMEM((units, width), F32),
            pltpu.VMEM((batch, rows, width), F32), pltpu.VMEM((batch, rows, width), BF16),
            pltpu.VMEM((SUB, units), F32), *[pltpu.VMEM(heads_t, BF16)] * 4, *[pltpu.VMEM(per_row, F32)] * 2,
            pltpu.VMEM((len(HEADS), rows, seq), F32), pltpu.VMEM((len(HEADS), rows, LANES), F32),
            pltpu.SemaphoreType.DMA((8,)),
        ],
        compiler_params=pltpu.CompilerParams(collective_id=1, has_side_effects=True, vmem_limit_bytes=VMEM_LIMIT),
    )(d_out, x_mid, z.reshape(batch, blocks, rows, units), w1, w2, q_t, k_t, v_t, gain.reshape(1, width), bias.reshape(1, width))


def attn_kernel(n_tp, scale, dx1_hbm, xi_hbm, q_hbm, k_hbm, v_hbm, ctxt_hbm, ctx_hbm, lse_hbm, wqkv_hbm, wo_hbm,
                gain_ref, bias_ref, vec_in,
                dx_hbm, dwqkv_hbm, dwo_hbm, dbqkv_ref, vecs_ref,
                mb, m_ss, m_rs, hb, h_ss, h_rs, p_out, p_in, sums, fin, transit, rs_ss, rs_rs,
                q_t, k_t, v_t, ctx_t, ctx, lse, wqkv, wo, dqkv, dk_acc, dv_acc, dq_acc,
                own, xi, dwqkv, dwo, vacc, vsend, vrecv, vring, lsem, v_ss, v_rs):
    place = Place(n_tp)
    rows, width = dx1_hbm.shape[1:]
    place.enter((place.partner, place.right, place.left, place.far))
    mg = Gather(place, dx1_hbm, mb, m_ss, m_rs)
    hg = Gather(place, hb.at[0], hb, h_ss, h_rs)
    sc = Scatter(place, p_out, p_in, sums, fin, transit, rs_ss, rs_rs)
    for b in BATCH:
        mg.start_own(b)
    loads = start_copies(((dx1_hbm, mb.at[0]), (wo_hbm, wo), (q_hbm, q_t), (k_hbm, k_t), (v_hbm, v_t), (ctx_hbm, ctx),
                          (lse_hbm, lse), (ctxt_hbm, ctx_t), (wqkv_hbm, wqkv), (xi_hbm, xi)), lsem)
    clear(dwqkv, dwo, dk_acc, dv_acc, vacc, vsend)
    for load in loads:
        load.wait()
    exp_scale = scale * LOG2E
    dim = LANES // len(HEADS)

    def attend(r, p, b):
        mid, blk = mb[CORES * r + p, b], place.block(r, p)
        qs = span(blk, rows)
        dwo[...] += mm(ctx_t[b, :, qs], mid, NN)
        dctx = mm(mid, wo[...], NT).astype(BF16)
        dctx_t = turn(dctx)
        qt = q_t[b, :, qs]
        q_h, d_h = split_heads(turn(qt)), split_heads(dctx)
        delta = [jnp.sum(v, axis=-1, keepdims=True) for v in split_heads(dctx.astype(F32) * ctx[b, blk])]
        lse_v = lse[b, blk]
        l_col = [lse_v[:, h * dim:h * dim + 1] for h in HEADS]
        last = blk // (TK // rows)
        clear(dq_acc)

        def tile(j, masked=False):
            ks = span(j, TK)
            kk, vv = k_t[b, :, ks], v_t[b, :, ks]
            for h in HEADS:
                hs = pl.ds(h * dim, dim)
                top = slice(h * dim, (h + 1) * dim)
                prob = jnp.exp2(mm(q_h[h], kk, NN) * exp_scale - l_col[h])
                if masked:
                    prob = jnp.where(visible(blk, j, rows), prob, 0.0)
                ds = (prob * (mm(d_h[h], vv, NN) - delta[h])).astype(BF16)
                dq_acc[h] += mm(ds, kk, NT)
                dk_acc[b, hs, ks] += mm(qt[top], ds, NN)
                dv_acc[b, hs, ks] += mm(dctx_t[top], prob.astype(BF16), NN)

        tile(last, True)
        loop(last, tile)
        dq = jnp.where(first_head(dq_acc.shape[1:]), dq_acc[0], dq_acc[1]) * scale
        dqkv[b, :LANES, qs] = turn(dq)

    def attend_own(b):
        mg.wait_partner(b)
        loop(CORES, lambda p: attend(0, p, b))

    def attend_near(b):
        mg.relay(b)
        for r in (R_RIGHT, R_LEFT):
            mg.wait_shared(r, b)
        loop(2 * CORES, lambda i: attend(R_RIGHT + 2 * (i // CORES), lax.rem(i, CORES), b))

    def partial_rows(r, p, b):
        return turn(dqkv[b, :, span(place.block(r, p), rows)])

    def reduce_out(r, b):
        lhs = partial_rows(r, 0, b)
        sc.to_partner(r, b).wait_recv()
        for ns in columns(width):
            sums[r - 1, b, :, ns] = (mm(lhs, wqkv[:, ns], NN) + p_in[r, b, :, ns].astype(F32)).astype(BF16)

    def attend_far(b):
        mg.relay_far(b)
        mg.wait_shared(R_FAR, b)
        loop(CORES, lambda p: attend(R_FAR, p, b))
        dqkv[b, LANES:2 * LANES] = (dk_acc[b] * scale).astype(BF16)
        dqkv[b, 2 * LANES:] = dv_acc[b].astype(BF16)

        def to_partner(i):
            r = lax.rem(R_FAR + i, place.chips)
            lhs = partial_rows(r, 1, b)
            for ns in columns(width):
                p_out[r, b, :, ns] = mm(lhs, wqkv[:, ns], NN).astype(BF16)
            sc.to_partner(r, b).start()

        loop(place.chips, to_partner)
        reduce_out(R_FAR, b)
        sc.send_far(b)
        loop(2, lambda i: reduce_out(R_RIGHT + 2 * i, b))
        sc.send_near(b)
        lhs = partial_rows(0, 0, b)
        sc.to_partner(0, b).wait_recv()
        for ns in columns(width):
            own[b, :, ns] = mm(lhs, wqkv[:, ns], NN) + p_in[0, b, :, ns].astype(F32)

    def dw_pair(r, b):
        def body(p):
            dwqkv[...] += mm(dqkv[b, :, span(place.block(r, p), rows)], hb[CORES * r + p, b], NN)
        loop(CORES, body)

    def dw_own(b):
        hg.wait_partner(b)
        dw_pair(0, b)

    def dw_near(b):
        def body(i):
            r = R_RIGHT + 2 * i
            hg.wait_shared(r, b)
            dw_pair(r, b)
        loop(2, body)

    def dw_far(b):
        hg.relay_far(b)
        hg.wait_shared(R_FAR, b)
        dw_pair(R_FAR, b)

    def back(b):
        sc.wait_final(b)

        def body(i):
            rs = span(i, STEP)
            grad = sc.total(own, b, rs)
            x_hat, inv_std = ln_stats(xi[b, rs].astype(F32))
            dx = (mb[0, b, rs].astype(F32) + ln_bwd(grad, x_hat, inv_std, gain_ref[...])).astype(BF16)
            xi[b, rs] = dx
            for k, v in enumerate((grad * x_hat, grad)):
                vacc[k] += fold8(v)
        loop(rows // STEP, body)

    loop(2, attend_own)
    normalize(xi, hb, gain_ref, bias_ref)
    loop(2, attend_near)
    hg.start_own(0)
    loop(2, attend_far)
    hg.start_own(1)
    loop(2, sc.send_last)
    hg.relay(0)
    loop(2, dw_own)
    ones = jnp.ones((SUB, dqkv.shape[2]), BF16)
    dbqkv_ref[...] = (mm(ones, dqkv[0], NT) + mm(ones, dqkv[1], NT))[:1]
    hg.relay(1)
    loop(2, dw_near)
    loop(2, back)
    stores = start_copies(((xi, dx_hbm), (dwo, dwo_hbm)), lsem)
    rows_in = [vacc[k] for k in range(vacc.shape[0])] + [vec_in[k] for k in range(vec_in.shape[0])]
    for k, v in enumerate(rows_in):
        vsend[k:k + 1] = jnp.sum(v, axis=0, keepdims=True)
    swap = remote(vsend, vrecv, v_ss.at[0], v_rs.at[n_tp], place.partner)
    swap.start()
    swap.wait_recv()
    vring[place.x] = vsend[...] + vrecv[...]
    ring = [remote(vring.at[place.x], vring.at[place.x], v_ss.at[r], v_rs.at[place.x], peer)
            for r, peer in zip(RING, (place.right, place.far, place.left))]
    for copy in ring:
        copy.start()
    loop(2, dw_far)
    stores += start_copies(((dwqkv, dwqkv_hbm),), lsem.at[pl.ds(2, 1)])
    for r in RING:
        other = lax.rem(place.x + r, place.chips)
        remote(vring.at[other], vring.at[other], v_ss.at[r], v_rs.at[other], place.right).wait_recv()
    vecs_ref[...] = functools.reduce(jnp.add, [vring[k] for k in range(vring.shape[0])])[:vecs_ref.shape[0]]
    swap.wait_send()
    for copy in ring:
        copy.wait_send()
    mg.finish()
    hg.finish()
    sc.finish()
    for store in stores:
        store.wait()


def attn_backward(n_tp, scale, dx1, x_in, q_t, k_t, v_t, ctx_t, ctx, lse, wqkv_t, wo, gain, bias, vec):
    batch, rows, width = dx1.shape
    seq = q_t.shape[2]
    any_spec = pl.BlockSpec(memory_space=pl.ANY)
    vm = pl.BlockSpec(memory_space=pltpu.VMEM)
    qkv_rows = wqkv_t.shape[0]
    vrow = pltpu.VMEM((SUB, width), F32)
    return pl.pallas_call(
        functools.partial(attn_kernel, n_tp, scale),
        name='attn_backward',
        out_shape=(jax.ShapeDtypeStruct((batch, rows, width), BF16), jax.ShapeDtypeStruct((qkv_rows, width), F32),
                   jax.ShapeDtypeStruct((LANES, width), F32), jax.ShapeDtypeStruct((1, qkv_rows), F32),
                   jax.ShapeDtypeStruct((6, width), F32)),
        in_specs=[any_spec] * 10 + [vm] * 3,
        out_specs=(any_spec, any_spec, any_spec, vm, vm),
        scratch_shapes=gather_scratch(rows, width) + gather_scratch(rows, width) + scatter_scratch(rows, width) + [
            *[pltpu.VMEM(q_t.shape, BF16)] * 4, *[pltpu.VMEM(ctx.shape, F32)] * 2,
            pltpu.VMEM((qkv_rows, width), BF16), pltpu.VMEM((LANES, width), BF16),
            pltpu.VMEM((batch, qkv_rows, seq), BF16), *[pltpu.VMEM((batch, LANES, seq), F32)] * 2,
            pltpu.VMEM((len(HEADS), rows, LANES), F32),
            pltpu.VMEM((batch, rows, width), F32), pltpu.VMEM((batch, rows, width), BF16),
            pltpu.VMEM((qkv_rows, width), F32), pltpu.VMEM((LANES, width), F32),
            pltpu.VMEM((2, SUB, width), F32), vrow, vrow, pltpu.VMEM((n_tp // CORES, SUB, width), F32),
            pltpu.SemaphoreType.DMA((10,)), pltpu.SemaphoreType.DMA((4,)), pltpu.SemaphoreType.DMA((n_tp + 1,)),
        ],
        compiler_params=pltpu.CompilerParams(collective_id=2, has_side_effects=True, vmem_limit_bytes=VMEM_LIMIT),
    )(dx1, x_in, q_t, k_t, v_t, ctx_t, ctx, lse, wqkv_t, wo, gain.reshape(1, width), bias.reshape(1, width), vec)


def solution(mesh):
    n_tp = mesh.shape['tp']

    def local_backward(x_in, x_mid, d_out, q_saved, k_saved, v_saved, z_saved, ln1_gain, ln1_bias, ln2_gain, ln2_bias, w_qkv, w_proj, w_fc1, w_fc2):
        batch, seq, heads, dim = q_saved.shape
        width = x_in.shape[-1]
        scale = dim ** -0.5

        def feature_rows(a):
            return jnp.transpose(a, (0, 2, 3, 1)).reshape(batch, heads * dim, seq)

        q_t, k_t, v_t = feature_rows(q_saved), feature_rows(k_saved), feature_rows(v_saved)
        wqkv_t = jnp.transpose(w_qkv, (0, 2, 3, 1)).reshape(w_qkv.shape[0] * heads * dim, width)
        wo = w_proj.reshape(heads * dim, width)
        dx1, grad_wfc1, grad_wfc2, ctx_t, ctx, lse, db1, vec = mlp_backward(
            n_tp, scale * LOG2E, d_out, x_mid, z_saved, w_fc1, w_fc2, q_t, k_t, v_t, ln2_gain, ln2_bias)
        grad_x, dwqkv, dwo, dbqkv, grad_vecs = attn_backward(
            n_tp, scale, dx1, x_in, q_t, k_t, v_t, ctx_t, ctx, lse, wqkv_t, wo, ln1_gain, ln1_bias, vec)
        grad_wqkv = jnp.transpose(dwqkv.reshape(-1, heads, dim, width), (0, 3, 1, 2))
        grad_bqkv = dbqkv.reshape(-1, heads, dim)
        grad_wproj = dwo.reshape(heads, dim, width)
        return grad_x, grad_wqkv, grad_bqkv, grad_wproj, grad_wfc1, db1.reshape(-1), grad_wfc2, grad_vecs

    tok_spec = P('dp', 'tp', None)
    head_spec = P('dp', None, 'tp', None)
    in_specs = (tok_spec, tok_spec, tok_spec, head_spec, head_spec, head_spec, P('dp', None, 'tp'),
                P(None), P(None), P(None), P(None),
                P(None, None, 'tp', None), P('tp', None, None), P(None, 'tp'), P('tp', None))
    out_specs = (tok_spec, P('dp', None, 'tp', None), P('dp', 'tp', None), P(('dp', 'tp'), None, None),
                 P('dp', 'tp'), P(('dp', 'tp')), P(('dp', 'tp'), None), P('dp', None))
    return jax.shard_map(local_backward, mesh=mesh, in_specs=in_specs, out_specs=out_specs, check_vma=False)
```

```python
import functools

import jax
import jax.numpy as jnp
from jax import lax
from jax.experimental import pallas as pl
from jax.experimental.pallas import tpu as pltpu
from jax.sharding import PartitionSpec as P

LN_EPS = 1e-5
GELU_COEF = 0.044715
GELU_SCALE = 0.7978845608028654
LOG2E = 1.4426950408889634
MESH = pl.DeviceIdType.MESH
F32 = jnp.float32
BF16 = jnp.bfloat16
VMEM_LIMIT = 67043328

NN = (((1,), (0,)), ((), ()))
NT = (((1,), (1,)), ((), ()))
TN = (((0,), (0,)), ((), ()))

CORES = 2
BATCH = range(2)
HEADS = range(2)
RING = R_RIGHT, R_FAR, R_LEFT = 1, 2, 3
SLOT_P, SLOT_R, SLOT_F, SLOT_L, SLOT_END = 1, 2, 4, 6, 8
PARTNER, RIGHT, LEFT, FWD_R, FWD_L = range(5)
NEAR_R, NEAR_L, FAR_R, FAR_L, LAST_R, LAST_L = range(4, 10)
SUB = 8
LANES = 128
TK = 512
NC = 256
STEP = 64


def mm(a, b, dims):
    return lax.dot_general(a, b, dims, preferred_element_type=F32)


def loop(count, body):
    def run(i, carry):
        body(i)
        return carry
    lax.fori_loop(0, count, run, 0)


def fold8(v):
    return jnp.sum(v.reshape(v.shape[0] // SUB, SUB, v.shape[1]), axis=0)


def turn(v):
    return jnp.transpose(v.astype(F32)).astype(BF16)


def span(i, size):
    return pl.ds(pl.multiple_of(i * size, size), size)


def columns(width):
    return [pl.ds(n * NC, NC) for n in range(width // NC)]


def clear(*refs):
    for ref in refs:
        ref[...] = jnp.zeros_like(ref)


def ln_stats(rows):
    centered = rows - jnp.mean(rows, axis=-1, keepdims=True)
    inv_std = lax.rsqrt(jnp.mean(centered * centered, axis=-1, keepdims=True) + LN_EPS)
    return centered * inv_std, inv_std


def ln_bwd(grad, x_hat, inv_std, gain):
    grad_hat = grad * gain
    centered = grad_hat - jnp.mean(grad_hat, axis=-1, keepdims=True)
    return inv_std * (centered - x_hat * jnp.mean(grad_hat * x_hat, axis=-1, keepdims=True))


def normalize(src, dst, gain, bias):
    per = src.shape[1] // STEP

    def body(i):
        b, rs = i // per, span(lax.rem(i, per), STEP)
        x_hat, _ = ln_stats(src[b, rs].astype(F32))
        dst[0, b, rs] = (x_hat * gain[...] + bias[...]).astype(BF16)

    loop(len(BATCH) * per, body)


def start_copies(pairs, sems):
    copies = [pltpu.make_async_copy(s, d, sems.at[i]) for i, (s, d) in enumerate(pairs)]
    for copy in copies:
        copy.start()
    return copies


class Place:
    def __init__(self, n_tp):
        self.chips = n_tp // CORES
        me = lax.axis_index('tp')
        self.x = me // CORES
        self.c = lax.rem(me, CORES)
        self.partner = self.block(0, 1)
        self.right, self.far, self.left = [self.block(r, 0) for r in RING]

    def block(self, r, p):
        return lax.rem(self.x + r, self.chips) * CORES + lax.rem(self.c + p, CORES)

    def enter(self, peers):
        barrier = pltpu.get_barrier_semaphore()
        for peer in peers:
            pl.semaphore_signal(barrier, inc=1, device_id={'tp': peer}, device_id_type=MESH)
        pl.semaphore_wait(barrier, len(peers))


def remote(src, dst, ssem, rsem, peer):
    return pltpu.make_async_remote_copy(src_ref=src, dst_ref=dst, send_sem=ssem, recv_sem=rsem,
                                        device_id={'tp': peer}, device_id_type=MESH)


class Gather:
    def __init__(self, place, own, buf, ssem, rsem):
        self.place, self.own, self.buf, self.ssem, self.rsem = place, own, buf, ssem, rsem
        half = buf.shape[-2] // 2
        self.lo, self.hi = pl.ds(0, half), pl.ds(half, half)

    def _own(self, kind, slot, b, peer):
        return remote(self.own.at[b], self.buf.at[slot, b], self.ssem.at[kind, b], self.rsem.at[slot, b], peer)

    def to_partner(self, b):
        return self._own(PARTNER, SLOT_P, b, self.place.partner)

    def to_right(self, b):
        return self._own(RIGHT, SLOT_L, b, self.place.right)

    def to_left(self, b):
        return self._own(LEFT, SLOT_R, b, self.place.left)

    def fwd_right(self, b):
        return remote(self.buf.at[SLOT_L, b, self.lo], self.buf.at[SLOT_F, b, self.lo],
                      self.ssem.at[FWD_R, b], self.rsem.at[SLOT_F, b], self.place.right)

    def fwd_left(self, b):
        return remote(self.buf.at[SLOT_R, b, self.hi], self.buf.at[SLOT_F, b, self.hi],
                      self.ssem.at[FWD_L, b], self.rsem.at[SLOT_END, b], self.place.left)

    def share(self, r, b):
        slot = CORES * r
        return remote(self.buf.at[slot, b], self.buf.at[slot + 1, b], self.ssem.at[FWD_L + r, b], self.rsem.at[slot + 1, b],
                      self.place.partner)

    def start_own(self, b):
        self.to_right(b).start()
        self.to_left(b).start()
        self.to_partner(b).start()

    def relay(self, b):
        self.to_right(b).wait_recv()
        self.fwd_right(b).start()
        self.to_left(b).wait_recv()
        self.fwd_left(b).start()
        self.share(R_LEFT, b).start()
        self.share(R_RIGHT, b).start()

    def relay_far(self, b):
        self.fwd_right(b).wait_recv()
        self.fwd_left(b).wait_recv()
        self.share(R_FAR, b).start()

    def wait_shared(self, r, b):
        self.share(r, b).wait_recv()

    def wait_partner(self, b):
        self.to_partner(b).wait_recv()

    def finish(self):
        for b in BATCH:
            for copy in (self.to_partner(b), self.to_right(b), self.to_left(b), self.fwd_right(b), self.fwd_left(b),
                         *(self.share(r, b) for r in RING)):
                copy.wait_send()


class Scatter:
    def __init__(self, place, p_out, p_in, sums, fin, transit, ssem, rsem):
        self.place = place
        self.p_out, self.p_in, self.sums, self.fin, self.transit = p_out, p_in, sums, fin, transit
        self.ssem, self.rsem = ssem, rsem
        half = sums.shape[-2] // 2
        self.lo, self.hi = pl.ds(0, half), pl.ds(half, half)

    def to_partner(self, r, b):
        return remote(self.p_out.at[r, b], self.p_in.at[r, b], self.ssem.at[r, b], self.rsem.at[r, b], self.place.partner)

    def _hop(self, kind, src, dst, b, peer):
        return remote(src, dst, self.ssem.at[kind, b], self.rsem.at[kind, b], peer)

    def near_right(self, b):
        return self._hop(NEAR_R, self.sums.at[0, b, self.hi], self.fin.at[0, b, self.hi], b, self.place.right)

    def near_left(self, b):
        return self._hop(NEAR_L, self.sums.at[2, b, self.lo], self.fin.at[1, b, self.lo], b, self.place.left)

    def far_right(self, b):
        return self._hop(FAR_R, self.sums.at[1, b, self.lo], self.transit.at[0, b], b, self.place.right)

    def far_left(self, b):
        return self._hop(FAR_L, self.sums.at[1, b, self.hi], self.transit.at[1, b], b, self.place.left)

    def last_right(self, b):
        return self._hop(LAST_R, self.sums.at[0, b, self.lo], self.fin.at[0, b, self.lo], b, self.place.right)

    def last_left(self, b):
        return self._hop(LAST_L, self.sums.at[2, b, self.hi], self.fin.at[1, b, self.hi], b, self.place.left)

    def send_near(self, b):
        self.near_right(b).start()
        self.near_left(b).start()

    def send_far(self, b):
        self.far_right(b).start()
        self.far_left(b).start()

    def send_last(self, b):
        for arrived, slot, lane, rows, onward in ((self.far_right, 0, 0, self.lo, self.last_right),
                                                  (self.far_left, 2, 1, self.hi, self.last_left)):
            arrived(b).wait_recv()
            self.sums[slot, b, rows] = (self.sums[slot, b, rows].astype(F32) + self.transit[lane, b].astype(F32)).astype(BF16)
            onward(b).start()

    def wait_final(self, b):
        for copy in (self.near_right, self.near_left, self.last_right, self.last_left):
            copy(b).wait_recv()

    def total(self, own, b, rs):
        return own[b, rs] + self.fin[0, b, rs].astype(F32) + self.fin[1, b, rs].astype(F32)

    def finish(self):
        for b in BATCH:
            for r in (0, *RING):
                self.to_partner(r, b).wait_send()
            for copy in (self.near_right, self.near_left, self.far_right, self.far_left, self.last_right, self.last_left):
                copy(b).wait_send()


def scatter_scratch(rows, width):
    def buf(*lead):
        return pltpu.VMEM((*lead, len(BATCH), rows, width), BF16)
    return [buf(4), buf(4), buf(3), buf(2), pltpu.VMEM((2, len(BATCH), rows // 2, width), BF16),
            pltpu.SemaphoreType.DMA((10, 2)), pltpu.SemaphoreType.DMA((10, 2))]


def gather_scratch(rows, width):
    return [pltpu.VMEM((SLOT_END, len(BATCH), rows, width), BF16),
            pltpu.SemaphoreType.DMA((SLOT_END, 2)), pltpu.SemaphoreType.DMA((SLOT_END + 1, 2))]


def first_head(shape):
    return lax.broadcasted_iota(jnp.int32, shape, 1) < shape[1] // len(HEADS)


def split_heads(v):
    first, zero = first_head(v.shape), jnp.zeros_like(v)
    return [jnp.where(first, v, zero), jnp.where(first, zero, v)]


def visible(blk, j, rows):
    row_id = blk * rows + lax.broadcasted_iota(jnp.int32, (rows, TK), 0)
    return row_id >= j * TK + lax.broadcasted_iota(jnp.int32, (rows, TK), 1)


def attn_fwd_block(b, blk, q_t, k_t, v_t, ctx_t, ctx, lse, s_buf, m_buf, scale):
    rows = ctx.shape[2]
    qs = span(blk, rows)
    last = blk // (TK // rows)
    q_h = split_heads(turn(q_t[b, :, qs]))

    def fold(f, v):
        parts = [v[:, i:i + LANES] for i in range(0, TK, LANES)]
        return functools.reduce(f, parts)

    def score(j, masked=False):
        kk = k_t[b, :, span(j, TK)]
        for h in HEADS:
            s = mm(q_h[h], kk, NN) * scale
            if masked:
                s = jnp.where(visible(blk, j, rows), s, -1e30)
            s_buf[h, :, span(j, TK)] = s
            top = fold(jnp.maximum, s)
            m_buf[h] = top if masked else jnp.maximum(m_buf[h], top)

    score(last, True)
    loop(last, score)
    m_col = [jnp.max(m_buf[h], axis=-1, keepdims=True) for h in HEADS]
    clear(m_buf)

    def total(j):
        for h in HEADS:
            m_buf[h] += fold(jnp.add, jnp.exp2(s_buf[h, :, span(j, TK)] - m_col[h]))

    loop(last + 1, total)
    l_col = [m_col[h] + jnp.log2(jnp.sum(m_buf[h], axis=-1, keepdims=True)) for h in HEADS]
    clear(m_buf)

    def weigh(j):
        vv = v_t[b, :, span(j, TK)]
        for h in HEADS:
            m_buf[h] += mm(jnp.exp2(s_buf[h, :, span(j, TK)] - l_col[h]).astype(BF16), vv, NT)

    loop(last + 1, weigh)
    first = first_head(m_buf.shape[1:])
    out = jnp.where(first, m_buf[0], m_buf[1])
    ctx[b, blk] = out
    lse[b, blk] = jnp.where(first, *l_col)
    ctx_t[b, :, qs] = turn(out)


def mlp_kernel(n_tp, scale, dy_hbm, xm_hbm, z_hbm, w1_hbm, w2_hbm, q_hbm, k_hbm, v_hbm, gain_ref, bias_ref,
               dx1_hbm, dw1_hbm, dw2_hbm, ctxt_hbm, ctx_hbm, lse_hbm, db1_ref, vec_ref,
               dyb, dy_ss, dy_rs, hb, h_ss, h_rs, p_out, p_in, sums, fin, transit, rs_ss, rs_rs,
               z, w1, w2, dw1, dw2, own, xm, db1, q_t, k_t, v_t, ctx_t, ctx, lse, s_buf, m_buf, lsem):
    place = Place(n_tp)
    rows, width = dy_hbm.shape[1:]
    units = w2.shape[0]
    blocks = ctx.shape[1]
    place.enter((place.partner, place.right, place.left))
    dyg = Gather(place, dy_hbm, dyb, dy_ss, dy_rs)
    hg = Gather(place, hb.at[0], hb, h_ss, h_rs)
    sc = Scatter(place, p_out, p_in, sums, fin, transit, rs_ss, rs_rs)
    for b in BATCH:
        dyg.start_own(b)
    loads = start_copies(((xm_hbm, xm), (dy_hbm, dyb.at[0]), (w2_hbm, w2), (z_hbm, z), (w1_hbm, w1),
                          (q_hbm, q_t), (k_hbm, k_t), (v_hbm, v_t)), lsem)
    clear(dw1, dw2, db1, vec_ref)
    loads[0].wait()
    normalize(xm, hb, gain_ref, bias_ref)
    for load in loads[1:]:
        load.wait()

    def attend(lo, count):
        def body(i):
            i = lo + i
            attn_fwd_block(i // blocks, lax.rem(i, blocks), q_t, k_t, v_t, ctx_t, ctx, lse, s_buf, m_buf, scale)
        loop(count, body)

    def pre_piece(r, p, b):
        dy, blk = dyb[CORES * r + p, b], place.block(r, p)
        for fs in columns(units):
            act = mm(dy, w2[fs, :], NT)
            zf = z[b, blk, :, fs].astype(F32)
            t = jnp.tanh(GELU_SCALE * (zf + GELU_COEF * zf * zf * zf))
            half_t = 0.5 * (1.0 + t)
            slope = half_t + 0.5 * zf * (1.0 - t * t) * GELU_SCALE * (1.0 + 3.0 * GELU_COEF * zf * zf)
            u = (zf * half_t).astype(BF16)
            dzv = (act * slope).astype(BF16)
            z[b, blk, :, fs] = dzv
            db1[:, fs] += fold8(dzv.astype(F32))
            dw2[fs, :] += mm(u, dy, TN)
        return z[b, blk]

    def pair(r, b, put):
        dz = pre_piece(r, 1, b)
        for ns in columns(width):
            p_out[r, b, :, ns] = mm(dz, w1[ns, :], NT).astype(BF16)
        sc.to_partner(r, b).start()
        dz = pre_piece(r, 0, b)
        sc.to_partner(r, b).wait_recv()
        for ns in columns(width):
            put(ns, mm(dz, w1[ns, :], NT) + p_in[r, b, :, ns].astype(F32))

    def pair_out(r, b):
        dyg.wait_shared(r, b)

        def put(ns, v):
            sums[r - 1, b, :, ns] = v.astype(BF16)
        pair(r, b, put)

    def own_body(b):
        dyg.wait_partner(b)

        def put(ns, v):
            own[b, :, ns] = v
        pair(0, b, put)

    def near_body(b):
        dyg.relay(b)
        loop(2, lambda i: pair_out(R_RIGHT + 2 * i, b))
        sc.send_near(b)
        attend(2 * b, 2)

    def far_body(b):
        dyg.relay_far(b)
        pair_out(R_FAR, b)
        sc.send_far(b)
        hg.start_own(b)

    def dw1_pair(r, b):
        def body(p):
            dw1[...] += mm(hb[CORES * r + p, b], z[b, place.block(r, p)], TN)
        loop(CORES, body)

    def dw1_own(b):
        hg.wait_partner(b)
        dw1_pair(0, b)

    def dw1_near(b):
        def body(i):
            r = R_RIGHT + 2 * i
            hg.wait_shared(r, b)
            dw1_pair(r, b)
        loop(2, body)

    def dw1_far(b):
        hg.relay_far(b)
        hg.wait_shared(R_FAR, b)
        dw1_pair(R_FAR, b)

    def back(b):
        sc.wait_final(b)

        def body(i):
            rs = span(i, STEP)
            grad = sc.total(own, b, rs)
            x_hat, inv_std = ln_stats(xm[b, rs].astype(F32))
            dyf = dyb[0, b, rs].astype(F32)
            dx1 = (dyf + ln_bwd(grad, x_hat, inv_std, gain_ref[...])).astype(BF16)
            xm[b, rs] = dx1
            for k, v in enumerate((grad * x_hat, grad, dx1.astype(F32), dyf)):
                vec_ref[k] += fold8(v)
        loop(rows // STEP, body)

    loop(2, own_body)
    loop(2, near_body)
    loop(2, far_body)
    rest = 2 * blocks - 4
    attend(4, rest)
    ctx_stores = start_copies(((ctx_t, ctxt_hbm), (ctx, ctx_hbm), (lse, lse_hbm)), lsem)
    loop(2, sc.send_last)
    hg.relay(0)
    loop(2, dw1_own)
    hg.relay(1)
    loop(2, dw1_near)
    loop(2, back)
    for store in ctx_stores:
        store.wait()
    stores = start_copies(((xm, dx1_hbm), (dw2, dw2_hbm)), lsem)
    db1_ref[...] = jnp.sum(db1[...], axis=0, keepdims=True)
    loop(2, dw1_far)
    for store in stores:
        store.wait()
    stores = start_copies(((dw1, dw1_hbm),), lsem)
    dyg.finish()
    hg.finish()
    sc.finish()
    stores[0].wait()


def mlp_backward(n_tp, scale, d_out, x_mid, z, w1, w2, q_t, k_t, v_t, gain, bias):
    batch, rows, width = d_out.shape
    units = w2.shape[0]
    seq = q_t.shape[2]
    blocks = seq // rows
    any_spec = pl.BlockSpec(memory_space=pl.ANY)
    vm = pl.BlockSpec(memory_space=pltpu.VMEM)
    heads_t = (batch, LANES, seq)
    per_row = (batch, blocks, rows, LANES)
    return pl.pallas_call(
        functools.partial(mlp_kernel, n_tp, scale),
        name='mlp_backward',
        out_shape=(jax.ShapeDtypeStruct((batch, rows, width), BF16), jax.ShapeDtypeStruct((width, units), F32),
                   jax.ShapeDtypeStruct((units, width), F32), jax.ShapeDtypeStruct(heads_t, BF16),
                   jax.ShapeDtypeStruct(per_row, F32), jax.ShapeDtypeStruct(per_row, F32),
                   jax.ShapeDtypeStruct((1, units), F32), jax.ShapeDtypeStruct((4, SUB, width), F32)),
        in_specs=[any_spec] * 8 + [vm] * 2,
        out_specs=(*[any_spec] * 6, vm, vm),
        scratch_shapes=gather_scratch(rows, width) + gather_scratch(rows, width) + scatter_scratch(rows, width) + [
            pltpu.VMEM((batch, blocks, rows, units), BF16),
            pltpu.VMEM((width, units), BF16), pltpu.VMEM((units, width), BF16),
            pltpu.VMEM((width, units), F32), pltpu.VMEM((units, width), F32),
            pltpu.VMEM((batch, rows, width), F32), pltpu.VMEM((batch, rows, width), BF16),
            pltpu.VMEM((SUB, units), F32), *[pltpu.VMEM(heads_t, BF16)] * 4, *[pltpu.VMEM(per_row, F32)] * 2,
            pltpu.VMEM((len(HEADS), rows, seq), F32), pltpu.VMEM((len(HEADS), rows, LANES), F32),
            pltpu.SemaphoreType.DMA((8,)),
        ],
        compiler_params=pltpu.CompilerParams(collective_id=1, has_side_effects=True, vmem_limit_bytes=VMEM_LIMIT),
    )(d_out, x_mid, z.reshape(batch, blocks, rows, units), w1, w2, q_t, k_t, v_t, gain.reshape(1, width), bias.reshape(1, width))


def attn_kernel(n_tp, scale, dx1_hbm, xi_hbm, q_hbm, k_hbm, v_hbm, ctxt_hbm, ctx_hbm, lse_hbm, wqkv_hbm, wo_hbm,
                gain_ref, bias_ref, vec_in,
                dx_hbm, dwqkv_hbm, dwo_hbm, dbqkv_ref, vecs_ref,
                mb, m_ss, m_rs, hb, h_ss, h_rs, p_out, p_in, sums, fin, transit, rs_ss, rs_rs,
                q_t, k_t, v_t, ctx_t, ctx, lse, wqkv, wo, dqkv, dk_acc, dv_acc, dq_acc,
                own, xi, dwqkv, dwo, vacc, vsend, vrecv, vring, lsem, v_ss, v_rs):
    place = Place(n_tp)
    rows, width = dx1_hbm.shape[1:]
    place.enter((place.partner, place.right, place.left, place.far))
    mg = Gather(place, dx1_hbm, mb, m_ss, m_rs)
    hg = Gather(place, hb.at[0], hb, h_ss, h_rs)
    sc = Scatter(place, p_out, p_in, sums, fin, transit, rs_ss, rs_rs)
    for b in BATCH:
        mg.start_own(b)
    loads = start_copies(((dx1_hbm, mb.at[0]), (wo_hbm, wo), (q_hbm, q_t), (k_hbm, k_t), (v_hbm, v_t), (ctx_hbm, ctx),
                          (lse_hbm, lse), (ctxt_hbm, ctx_t), (wqkv_hbm, wqkv), (xi_hbm, xi)), lsem)
    clear(dwqkv, dwo, dk_acc, dv_acc, vacc, vsend)
    for load in loads:
        load.wait()
    exp_scale = scale * LOG2E
    dim = LANES // len(HEADS)

    def attend(r, p, b):
        mid, blk = mb[CORES * r + p, b], place.block(r, p)
        qs = span(blk, rows)
        dwo[...] += mm(ctx_t[b, :, qs], mid, NN)
        dctx = mm(mid, wo[...], NT).astype(BF16)
        dctx_t = turn(dctx)
        qt = q_t[b, :, qs]
        q_h, d_h = split_heads(turn(qt)), split_heads(dctx)
        delta = [jnp.sum(v, axis=-1, keepdims=True) for v in split_heads(dctx.astype(F32) * ctx[b, blk])]
        lse_v = lse[b, blk]
        l_col = [lse_v[:, h * dim:h * dim + 1] for h in HEADS]
        last = blk // (TK // rows)
        clear(dq_acc)

        def tile(j, masked=False):
            ks = span(j, TK)
            kk, vv = k_t[b, :, ks], v_t[b, :, ks]
            for h in HEADS:
                hs = pl.ds(h * dim, dim)
                top = slice(h * dim, (h + 1) * dim)
                prob = jnp.exp2(mm(q_h[h], kk, NN) * exp_scale - l_col[h])
                if masked:
                    prob = jnp.where(visible(blk, j, rows), prob, 0.0)
                ds = (prob * (mm(d_h[h], vv, NN) - delta[h])).astype(BF16)
                dq_acc[h] += mm(ds, kk, NT)
                dk_acc[b, hs, ks] += mm(qt[top], ds, NN)
                dv_acc[b, hs, ks] += mm(dctx_t[top], prob.astype(BF16), NN)

        tile(last, True)
        loop(last, tile)
        dq = jnp.where(first_head(dq_acc.shape[1:]), dq_acc[0], dq_acc[1]) * scale
        dqkv[b, :LANES, qs] = turn(dq)

    def attend_own(i):
        b, p = i // CORES, lax.rem(i, CORES)

        @pl.when(p == 0)
        def _():
            mg.wait_partner(b)

        @pl.when(i == len(BATCH) * CORES - 1)
        def _():
            mg.relay(0)
        attend(0, p, b)

    def attend_near(b):
        for r in (R_RIGHT, R_LEFT):
            mg.wait_shared(r, b)

        def body(i):
            @pl.when((i == 2 * CORES - 1) & (b == 0))
            def _():
                mg.relay(1)
                hg.start_own(0)
            attend(R_RIGHT + 2 * (i // CORES), lax.rem(i, CORES), b)
        loop(2 * CORES, body)

    def partial_rows(r, p, b):
        return turn(dqkv[b, :, span(place.block(r, p), rows)])

    def reduce_out(r, b):
        lhs = partial_rows(r, 0, b)
        sc.to_partner(r, b).wait_recv()
        for ns in columns(width):
            sums[r - 1, b, :, ns] = (mm(lhs, wqkv[:, ns], NN) + p_in[r, b, :, ns].astype(F32)).astype(BF16)

    def attend_far(b):
        @pl.when(b == 0)
        def _():
            mg.relay_far(0)
        mg.wait_shared(R_FAR, b)
        loop(CORES, lambda p: attend(R_FAR, p, b))

        @pl.when(b == 1)
        def _():
            sc.send_last(0)
        dqkv[b, LANES:2 * LANES] = (dk_acc[b] * scale).astype(BF16)
        dqkv[b, 2 * LANES:] = dv_acc[b].astype(BF16)

        def to_partner(i):
            r = lax.rem(R_FAR + i, place.chips)
            lhs = partial_rows(r, 1, b)
            for ns in columns(width):
                p_out[r, b, :, ns] = mm(lhs, wqkv[:, ns], NN).astype(BF16)
            sc.to_partner(r, b).start()

        loop(place.chips, to_partner)
        reduce_out(R_FAR, b)
        sc.send_far(b)
        loop(2, lambda i: reduce_out(R_RIGHT + 2 * i, b))
        sc.send_near(b)
        lhs = partial_rows(0, 0, b)
        sc.to_partner(0, b).wait_recv()
        for ns in columns(width):
            own[b, :, ns] = mm(lhs, wqkv[:, ns], NN) + p_in[0, b, :, ns].astype(F32)

    def dw_pair(r, b):
        def body(p):
            dwqkv[...] += mm(dqkv[b, :, span(place.block(r, p), rows)], hb[CORES * r + p, b], NN)
        loop(CORES, body)

    def dw_own(b):
        hg.wait_partner(b)
        dw_pair(0, b)

    def dw_near(b):
        def body(i):
            r = R_RIGHT + 2 * i
            hg.wait_shared(r, b)
            dw_pair(r, b)
        loop(2, body)

    def dw_far(b):
        hg.relay_far(b)
        hg.wait_shared(R_FAR, b)
        dw_pair(R_FAR, b)

    def back(b):
        sc.wait_final(b)

        def body(i):
            rs = span(i, STEP)
            grad = sc.total(own, b, rs)
            x_hat, inv_std = ln_stats(xi[b, rs].astype(F32))
            dx = (mb[0, b, rs].astype(F32) + ln_bwd(grad, x_hat, inv_std, gain_ref[...])).astype(BF16)
            xi[b, rs] = dx
            for k, v in enumerate((grad * x_hat, grad)):
                vacc[k] += fold8(v)
        loop(rows // STEP, body)

    def batch(b):
        @pl.when(b == 1)
        def _():
            mg.relay_far(1)
            hg.start_own(1)
        attend_near(b)
        attend_far(b)

    normalize(xi, hb, gain_ref, bias_ref)
    loop(len(BATCH) * CORES, attend_own)
    loop(2, batch)
    hg.relay(0)
    loop(2, dw_own)
    ones = jnp.ones((SUB, dqkv.shape[2]), BF16)
    dbqkv_ref[...] = (mm(ones, dqkv[0], NT) + mm(ones, dqkv[1], NT))[:1]
    sc.send_last(1)
    hg.relay(1)
    loop(2, dw_near)
    loop(2, back)
    stores = start_copies(((xi, dx_hbm), (dwo, dwo_hbm)), lsem)
    rows_in = [vacc[k] for k in range(vacc.shape[0])] + [vec_in[k] for k in range(vec_in.shape[0])]
    for k, v in enumerate(rows_in):
        vsend[k:k + 1] = jnp.sum(v, axis=0, keepdims=True)
    swap = remote(vsend, vrecv, v_ss.at[0], v_rs.at[n_tp], place.partner)
    swap.start()
    swap.wait_recv()
    vring[place.x] = vsend[...] + vrecv[...]
    ring = [remote(vring.at[place.x], vring.at[place.x], v_ss.at[r], v_rs.at[place.x], peer)
            for r, peer in zip(RING, (place.right, place.far, place.left))]
    for copy in ring:
        copy.start()
    loop(2, dw_far)
    stores += start_copies(((dwqkv, dwqkv_hbm),), lsem.at[pl.ds(2, 1)])
    for r in RING:
        other = lax.rem(place.x + r, place.chips)
        remote(vring.at[other], vring.at[other], v_ss.at[r], v_rs.at[other], place.right).wait_recv()
    vecs_ref[...] = functools.reduce(jnp.add, [vring[k] for k in range(vring.shape[0])])[:vecs_ref.shape[0]]
    swap.wait_send()
    for copy in ring:
        copy.wait_send()
    mg.finish()
    hg.finish()
    sc.finish()
    for store in stores:
        store.wait()


def attn_backward(n_tp, scale, dx1, x_in, q_t, k_t, v_t, ctx_t, ctx, lse, wqkv_t, wo, gain, bias, vec):
    batch, rows, width = dx1.shape
    seq = q_t.shape[2]
    any_spec = pl.BlockSpec(memory_space=pl.ANY)
    vm = pl.BlockSpec(memory_space=pltpu.VMEM)
    qkv_rows = wqkv_t.shape[0]
    vrow = pltpu.VMEM((SUB, width), F32)
    return pl.pallas_call(
        functools.partial(attn_kernel, n_tp, scale),
        name='attn_backward',
        out_shape=(jax.ShapeDtypeStruct((batch, rows, width), BF16), jax.ShapeDtypeStruct((qkv_rows, width), F32),
                   jax.ShapeDtypeStruct((LANES, width), F32), jax.ShapeDtypeStruct((1, qkv_rows), F32),
                   jax.ShapeDtypeStruct((6, width), F32)),
        in_specs=[any_spec] * 10 + [vm] * 3,
        out_specs=(any_spec, any_spec, any_spec, vm, vm),
        scratch_shapes=gather_scratch(rows, width) + gather_scratch(rows, width) + scatter_scratch(rows, width) + [
            *[pltpu.VMEM(q_t.shape, BF16)] * 4, *[pltpu.VMEM(ctx.shape, F32)] * 2,
            pltpu.VMEM((qkv_rows, width), BF16), pltpu.VMEM((LANES, width), BF16),
            pltpu.VMEM((batch, qkv_rows, seq), BF16), *[pltpu.VMEM((batch, LANES, seq), F32)] * 2,
            pltpu.VMEM((len(HEADS), rows, LANES), F32),
            pltpu.VMEM((batch, rows, width), F32), pltpu.VMEM((batch, rows, width), BF16),
            pltpu.VMEM((qkv_rows, width), F32), pltpu.VMEM((LANES, width), F32),
            pltpu.VMEM((2, SUB, width), F32), vrow, vrow, pltpu.VMEM((n_tp // CORES, SUB, width), F32),
            pltpu.SemaphoreType.DMA((10,)), pltpu.SemaphoreType.DMA((4,)), pltpu.SemaphoreType.DMA((n_tp + 1,)),
        ],
        compiler_params=pltpu.CompilerParams(collective_id=2, has_side_effects=True, vmem_limit_bytes=VMEM_LIMIT),
    )(dx1, x_in, q_t, k_t, v_t, ctx_t, ctx, lse, wqkv_t, wo, gain.reshape(1, width), bias.reshape(1, width), vec)


def place_results(big, small):
    pieces = 4

    def kernel(*refs):
        count, rest = len(big), len(small)
        src, small_in = refs[:count], refs[count:count + rest]
        dst, small_out = refs[count + rest:2 * count + rest], refs[2 * count + rest:2 * (count + rest)]
        bufs, sem_in, sem_out = refs[2 * (count + rest):-2], refs[-2], refs[-1]
        moves = []
        for i, buf in enumerate(bufs):
            step = buf.shape[0] // pieces
            for j in range(pieces):
                rs = pl.ds(j * step, step)
                moves.append((pltpu.make_async_copy(src[i].at[rs], buf.at[rs], sem_in.at[i, j]),
                              pltpu.make_async_copy(buf.at[rs], dst[i].at[rs], sem_out.at[i, j])))
        for fetch, _ in moves:
            fetch.start()
        for ref_in, ref_out in zip(small_in, small_out):
            ref_out[...] = ref_in[...]
        for fetch, put in moves:
            fetch.wait()
            put.start()
        for _, put in moves:
            put.wait()

    any_spec = pl.BlockSpec(memory_space=pl.ANY)
    vm = pl.BlockSpec(memory_space=pltpu.VMEM)
    return pl.pallas_call(
        kernel,
        name='place_results',
        out_shape=[jax.ShapeDtypeStruct(v.shape, v.dtype) for v in (*big, *small)],
        in_specs=[any_spec] * len(big) + [vm] * len(small),
        out_specs=[any_spec] * len(big) + [vm] * len(small),
        scratch_shapes=[pltpu.VMEM(v.shape, v.dtype) for v in big] + [pltpu.SemaphoreType.DMA((len(big), pieces))] * 2,
        compiler_params=pltpu.CompilerParams(vmem_limit_bytes=VMEM_LIMIT),
    )(*big, *small)


def solution(mesh):
    n_tp = mesh.shape['tp']

    def local_backward(x_in, x_mid, d_out, q_saved, k_saved, v_saved, z_saved, ln1_gain, ln1_bias, ln2_gain, ln2_bias, w_qkv, w_proj, w_fc1, w_fc2):
        batch, seq, heads, dim = q_saved.shape
        width = x_in.shape[-1]
        scale = dim ** -0.5

        def feature_rows(a):
            return jnp.transpose(a, (0, 2, 3, 1)).reshape(batch, heads * dim, seq)

        q_t, k_t, v_t = feature_rows(q_saved), feature_rows(k_saved), feature_rows(v_saved)
        wqkv_t = jnp.transpose(w_qkv, (0, 2, 3, 1)).reshape(w_qkv.shape[0] * heads * dim, width)
        wo = w_proj.reshape(heads * dim, width)
        dx1, grad_wfc1, grad_wfc2, ctx_t, ctx, lse, db1, vec = mlp_backward(
            n_tp, scale * LOG2E, d_out, x_mid, z_saved, w_fc1, w_fc2, q_t, k_t, v_t, ln2_gain, ln2_bias)
        grad_x, dwqkv, dwo, dbqkv, grad_vecs = attn_backward(
            n_tp, scale, dx1, x_in, q_t, k_t, v_t, ctx_t, ctx, lse, wqkv_t, wo, ln1_gain, ln1_bias, vec)
        grad_x, grad_wfc1, grad_wfc2, dwqkv, dwo, db1, dbqkv, grad_vecs = place_results(
            (grad_x.reshape(batch * x_in.shape[1], width), grad_wfc1, grad_wfc2, dwqkv, dwo), (db1, dbqkv, grad_vecs))
        grad_x = grad_x.reshape(x_in.shape)
        grad_wqkv = jnp.transpose(dwqkv.reshape(-1, heads, dim, width), (0, 3, 1, 2))
        grad_bqkv = dbqkv.reshape(-1, heads, dim)
        grad_wproj = dwo.reshape(heads, dim, width)
        return grad_x, grad_wqkv, grad_bqkv, grad_wproj, grad_wfc1, db1.reshape(-1), grad_wfc2, grad_vecs

    tok_spec = P('dp', 'tp', None)
    head_spec = P('dp', None, 'tp', None)
    in_specs = (tok_spec, tok_spec, tok_spec, head_spec, head_spec, head_spec, P('dp', None, 'tp'),
                P(None), P(None), P(None), P(None),
                P(None, None, 'tp', None), P('tp', None, None), P(None, 'tp'), P('tp', None))
    out_specs = (tok_spec, P('dp', None, 'tp', None), P('dp', 'tp', None), P(('dp', 'tp'), None, None),
                 P('dp', 'tp'), P(('dp', 'tp')), P(('dp', 'tp'), None), P('dp', None))
    return jax.shard_map(local_backward, mesh=mesh, in_specs=in_specs, out_specs=out_specs, check_vma=False)
```

```python
import functools

import jax
import jax.numpy as jnp
from jax import lax
from jax.experimental import pallas as pl
from jax.experimental.pallas import tpu as pltpu
from jax.sharding import PartitionSpec as P

LN_EPS = 1e-5
GELU_COEF = 0.044715
GELU_SCALE = 0.7978845608028654
LOG2E = 1.4426950408889634
MESH = pl.DeviceIdType.MESH
F32 = jnp.float32
BF16 = jnp.bfloat16
VMEM_LIMIT = 67043328

NN = (((1,), (0,)), ((), ()))
NT = (((1,), (1,)), ((), ()))
TN = (((0,), (0,)), ((), ()))

CORES = 2
BATCH = range(2)
HEADS = range(2)
RING = R_RIGHT, R_FAR, R_LEFT = 1, 2, 3
SLOT_P, SLOT_R, SLOT_F, SLOT_L, SLOT_END = 1, 2, 4, 6, 8
PARTNER, RIGHT, LEFT, FWD_R, FWD_L = range(5)
NEAR_R, NEAR_L, FAR_R, FAR_L, LAST_R, LAST_L = range(4, 10)
SUB = 8
LANES = 128
TK = 512
NC = 256
STEP = 64


def mm(a, b, dims):
    return lax.dot_general(a, b, dims, preferred_element_type=F32)


def loop(count, body):
    def run(i, carry):
        body(i)
        return carry
    lax.fori_loop(0, count, run, 0)


def fold8(v):
    return jnp.sum(v.reshape(v.shape[0] // SUB, SUB, v.shape[1]), axis=0)


def turn(v):
    return jnp.transpose(v.astype(F32)).astype(BF16)


def span(i, size):
    return pl.ds(pl.multiple_of(i * size, size), size)


def columns(width):
    return [pl.ds(n * NC, NC) for n in range(width // NC)]


def clear(*refs):
    for ref in refs:
        ref[...] = jnp.zeros_like(ref)


def ln_stats(rows):
    centered = rows - jnp.mean(rows, axis=-1, keepdims=True)
    inv_std = lax.rsqrt(jnp.mean(centered * centered, axis=-1, keepdims=True) + LN_EPS)
    return centered * inv_std, inv_std


def ln_bwd(grad, x_hat, inv_std, gain):
    grad_hat = grad * gain
    centered = grad_hat - jnp.mean(grad_hat, axis=-1, keepdims=True)
    return inv_std * (centered - x_hat * jnp.mean(grad_hat * x_hat, axis=-1, keepdims=True))


def normalize(src, dst, gain, bias, b):
    def body(i):
        rs = span(i, STEP)
        x_hat, _ = ln_stats(src[b, rs].astype(F32))
        dst[0, b, rs] = (x_hat * gain[...] + bias[...]).astype(BF16)

    loop(src.shape[1] // STEP, body)


def start_copies(pairs, sems):
    copies = [pltpu.make_async_copy(s, d, sems.at[i]) for i, (s, d) in enumerate(pairs)]
    for copy in copies:
        copy.start()
    return copies


class Place:
    def __init__(self, n_tp):
        self.chips = n_tp // CORES
        me = lax.axis_index('tp')
        self.x = me // CORES
        self.c = lax.rem(me, CORES)
        self.partner = self.block(0, 1)
        self.right, self.far, self.left = [self.block(r, 0) for r in RING]

    def block(self, r, p):
        return lax.rem(self.x + r, self.chips) * CORES + lax.rem(self.c + p, CORES)

    def enter(self, peers):
        barrier = pltpu.get_barrier_semaphore()
        for peer in peers:
            pl.semaphore_signal(barrier, inc=1, device_id={'tp': peer}, device_id_type=MESH)
        pl.semaphore_wait(barrier, len(peers))


def remote(src, dst, ssem, rsem, peer):
    return pltpu.make_async_remote_copy(src_ref=src, dst_ref=dst, send_sem=ssem, recv_sem=rsem,
                                        device_id={'tp': peer}, device_id_type=MESH)


class Gather:
    def __init__(self, place, own, buf, ssem, rsem):
        self.place, self.own, self.buf, self.ssem, self.rsem = place, own, buf, ssem, rsem
        half = buf.shape[-2] // 2
        self.lo, self.hi = pl.ds(0, half), pl.ds(half, half)

    def _own(self, kind, slot, b, peer):
        return remote(self.own.at[b], self.buf.at[slot, b], self.ssem.at[kind, b], self.rsem.at[slot, b], peer)

    def to_partner(self, b):
        return self._own(PARTNER, SLOT_P, b, self.place.partner)

    def to_right(self, b):
        return self._own(RIGHT, SLOT_L, b, self.place.right)

    def to_left(self, b):
        return self._own(LEFT, SLOT_R, b, self.place.left)

    def fwd_right(self, b):
        return remote(self.buf.at[SLOT_L, b, self.lo], self.buf.at[SLOT_F, b, self.lo],
                      self.ssem.at[FWD_R, b], self.rsem.at[SLOT_F, b], self.place.right)

    def fwd_left(self, b):
        return remote(self.buf.at[SLOT_R, b, self.hi], self.buf.at[SLOT_F, b, self.hi],
                      self.ssem.at[FWD_L, b], self.rsem.at[SLOT_END, b], self.place.left)

    def share(self, r, b):
        slot = CORES * r
        return remote(self.buf.at[slot, b], self.buf.at[slot + 1, b], self.ssem.at[FWD_L + r, b], self.rsem.at[slot + 1, b],
                      self.place.partner)

    def start_own(self, b):
        self.to_right(b).start()
        self.to_left(b).start()
        self.to_partner(b).start()

    def relay(self, b):
        self.to_right(b).wait_recv()
        self.fwd_right(b).start()
        self.to_left(b).wait_recv()
        self.fwd_left(b).start()
        self.share(R_LEFT, b).start()
        self.share(R_RIGHT, b).start()

    def relay_far(self, b):
        self.fwd_right(b).wait_recv()
        self.fwd_left(b).wait_recv()
        self.share(R_FAR, b).start()

    def wait_shared(self, r, b):
        self.share(r, b).wait_recv()

    def wait_partner(self, b):
        self.to_partner(b).wait_recv()

    def drain_own(self, b):
        for copy in (self.to_partner, self.to_right, self.to_left):
            copy(b).wait_send()

    def drain_near(self, b):
        for copy in (self.fwd_right(b), self.fwd_left(b), self.share(R_RIGHT, b), self.share(R_LEFT, b)):
            copy.wait_send()

    def drain_far(self, b):
        self.share(R_FAR, b).wait_send()

    def drain(self, b):
        self.drain_own(b)
        self.drain_near(b)
        self.drain_far(b)


class Scatter:
    def __init__(self, place, p_out, p_in, sums, fin, transit, ssem, rsem):
        self.place = place
        self.p_out, self.p_in, self.sums, self.fin, self.transit = p_out, p_in, sums, fin, transit
        self.ssem, self.rsem = ssem, rsem
        half = sums.shape[-2] // 2
        self.lo, self.hi = pl.ds(0, half), pl.ds(half, half)

    def to_partner(self, r, b):
        return remote(self.p_out.at[r, b], self.p_in.at[r, b], self.ssem.at[r, b], self.rsem.at[r, b], self.place.partner)

    def _hop(self, kind, src, dst, b, peer):
        return remote(src, dst, self.ssem.at[kind, b], self.rsem.at[kind, b], peer)

    def near_right(self, b):
        return self._hop(NEAR_R, self.sums.at[0, b, self.hi], self.fin.at[0, b, self.hi], b, self.place.right)

    def near_left(self, b):
        return self._hop(NEAR_L, self.sums.at[2, b, self.lo], self.fin.at[1, b, self.lo], b, self.place.left)

    def far_right(self, b):
        return self._hop(FAR_R, self.sums.at[1, b, self.lo], self.transit.at[0, b], b, self.place.right)

    def far_left(self, b):
        return self._hop(FAR_L, self.sums.at[1, b, self.hi], self.transit.at[1, b], b, self.place.left)

    def last_right(self, b):
        return self._hop(LAST_R, self.sums.at[0, b, self.lo], self.fin.at[0, b, self.lo], b, self.place.right)

    def last_left(self, b):
        return self._hop(LAST_L, self.sums.at[2, b, self.hi], self.fin.at[1, b, self.hi], b, self.place.left)

    def send_near(self, b):
        self.near_right(b).start()
        self.near_left(b).start()

    def send_far(self, b):
        self.far_right(b).start()
        self.far_left(b).start()

    def send_last(self, b):
        for arrived, slot, lane, rows, onward in ((self.far_right, 0, 0, self.lo, self.last_right),
                                                  (self.far_left, 2, 1, self.hi, self.last_left)):
            arrived(b).wait_recv()
            self.sums[slot, b, rows] = (self.sums[slot, b, rows].astype(F32) + self.transit[lane, b].astype(F32)).astype(BF16)
            onward(b).start()

    def wait_final(self, b):
        for copy in (self.near_right, self.near_left, self.last_right, self.last_left):
            copy(b).wait_recv()

    def total(self, own, b, rs):
        return own[b, rs] + self.fin[0, b, rs].astype(F32) + self.fin[1, b, rs].astype(F32)

    def finish(self):
        for b in BATCH:
            for r in (0, *RING):
                self.to_partner(r, b).wait_send()
            for copy in (self.near_right, self.near_left, self.far_right, self.far_left, self.last_right, self.last_left):
                copy(b).wait_send()


def scatter_scratch(rows, width):
    def buf(*lead):
        return pltpu.VMEM((*lead, len(BATCH), rows, width), BF16)
    return [buf(4), buf(4), buf(3), buf(2), pltpu.VMEM((2, len(BATCH), rows // 2, width), BF16)]


def copy_sems(*counts):
    return [pltpu.SemaphoreType.DMA((count, len(BATCH))) for count in counts]


def first_head(shape):
    return lax.broadcasted_iota(jnp.int32, shape, 1) < shape[1] // len(HEADS)


def split_heads(v):
    first, zero = first_head(v.shape), jnp.zeros_like(v)
    return [jnp.where(first, v, zero), jnp.where(first, zero, v)]


def visible(blk, j, rows):
    row_id = blk * rows + lax.broadcasted_iota(jnp.int32, (rows, TK), 0)
    return row_id >= j * TK + lax.broadcasted_iota(jnp.int32, (rows, TK), 1)


def attn_fwd_block(b, blk, q_t, k_t, v_t, ctx_t, ctx, lse, s_buf, m_buf, scale):
    rows = ctx.shape[2]
    qs = span(blk, rows)
    last = blk // (TK // rows)
    q_h = split_heads(turn(q_t[b, :, qs]))

    def fold(f, v):
        parts = [v[:, i:i + LANES] for i in range(0, TK, LANES)]
        return functools.reduce(f, parts)

    def score(j, masked=False):
        kk = k_t[b, :, span(j, TK)]
        for h in HEADS:
            s = mm(q_h[h], kk, NN) * scale
            if masked:
                s = jnp.where(visible(blk, j, rows), s, -1e30)
            s_buf[h, :, span(j, TK)] = s
            top = fold(jnp.maximum, s)
            m_buf[h] = top if masked else jnp.maximum(m_buf[h], top)

    score(last, True)
    loop(last, score)
    m_col = [jnp.max(m_buf[h], axis=-1, keepdims=True) for h in HEADS]
    clear(m_buf)

    def total(j):
        for h in HEADS:
            m_buf[h] += fold(jnp.add, jnp.exp2(s_buf[h, :, span(j, TK)] - m_col[h]))

    loop(last + 1, total)
    l_col = [m_col[h] + jnp.log2(jnp.sum(m_buf[h], axis=-1, keepdims=True)) for h in HEADS]
    clear(m_buf)

    def weigh(j):
        vv = v_t[b, :, span(j, TK)]
        for h in HEADS:
            m_buf[h] += mm(jnp.exp2(s_buf[h, :, span(j, TK)] - l_col[h]).astype(BF16), vv, NT)

    loop(last + 1, weigh)
    first = first_head(m_buf.shape[1:])
    out = jnp.where(first, m_buf[0], m_buf[1])
    ctx[b, blk] = out
    lse_t = jnp.transpose(jnp.where(first, *l_col))
    for h in HEADS:
        top = h * (LANES // len(HEADS))
        lse[b, blk, h:h + 1] = lse_t[top:top + 1]
    ctx_t[b, :, qs] = turn(out)


def backward_kernel(n_tp, scale, dy_hbm, xm_hbm, z_hbm, w1_hbm, w2_hbm, q_hbm, k_hbm, v_hbm, xi_hbm, wqkv_hbm, wo_hbm,
                    gain2_ref, bias2_ref, gain1_ref, bias1_ref,
                    dx_hbm, dw1_hbm, dw2_hbm, dwqkv_hbm, dwo_hbm, db1_ref, dbqkv_ref, vecs_ref,
                    tok, hb, p_out, p_in, sums, fin, transit,
                    z, w1, w2, dw1, dw2, own, xm, xi, db1, q_t, k_t, v_t, ctx_t, ctx, lse, acc, head_acc,
                    wqkv, wo, dqkv, dwqkv, dwo, vacc, vsend, vrecv, vring,
                    dy_ss, dy_rs, h2_ss, h2_rs, dx_ss, dx_rs, h1_ss, h1_rs, rs2_ss, rs2_rs, rs1_ss, rs1_rs,
                    lsem, v_ss, v_rs, credit):
    place = Place(n_tp)
    rows, width = dy_hbm.shape[1:]
    units = w2.shape[0]
    blocks = ctx.shape[1]
    neighbours = (place.partner, place.right, place.left)
    place.enter((*neighbours, place.far))
    dyg = Gather(place, dy_hbm, tok, dy_ss, dy_rs)
    mg = Gather(place, tok.at[0], tok, dx_ss, dx_rs)
    h2g = Gather(place, hb.at[0], hb, h2_ss, h2_rs)
    h1g = Gather(place, hb.at[0], hb, h1_ss, h1_rs)
    sc2 = Scatter(place, p_out, p_in, sums, fin, transit, rs2_ss, rs2_rs)
    sc1 = Scatter(place, p_out, p_in, sums, fin, transit, rs1_ss, rs1_rs)
    for b in BATCH:
        dyg.start_own(b)
    loads = start_copies(((xm_hbm, xm), (dy_hbm, tok.at[0]), (w2_hbm, w2), (z_hbm, z), (w1_hbm, w1),
                          (q_hbm, q_t), (k_hbm, k_t), (v_hbm, v_t), (wo_hbm, wo), (wqkv_hbm, wqkv), (xi_hbm, xi)), lsem)
    clear(dw1, dw2, db1, vacc, vsend, dwqkv, dwo, lse)
    loads[0].wait()
    loop(2, functools.partial(normalize, xm, hb, gain2_ref, bias2_ref))
    for load in loads[1:]:
        load.wait()
    exp_scale = scale * LOG2E
    dim = LANES // len(HEADS)

    def recall(lo, count):
        def body(i):
            i = lo + i
            attn_fwd_block(i // blocks, lax.rem(i, blocks), q_t, k_t, v_t, ctx_t, ctx, lse, acc, head_acc, exp_scale)
        loop(count, body)

    def pre_piece(r, p, b):
        dy, blk = tok[CORES * r + p, b], place.block(r, p)
        for fs in columns(units):
            act = mm(dy, w2[fs, :], NT)
            zf = z[b, blk, :, fs].astype(F32)
            t = jnp.tanh(GELU_SCALE * (zf + GELU_COEF * zf * zf * zf))
            half_t = 0.5 * (1.0 + t)
            slope = half_t + 0.5 * zf * (1.0 - t * t) * GELU_SCALE * (1.0 + 3.0 * GELU_COEF * zf * zf)
            u = (zf * half_t).astype(BF16)
            dzv = (act * slope).astype(BF16)
            z[b, blk, :, fs] = dzv
            db1[:, fs] += fold8(dzv.astype(F32))
            dw2[fs, :] += mm(u, dy, TN)
        return z[b, blk]

    def pair(r, b, put):
        dz = pre_piece(r, 1, b)
        for ns in columns(width):
            p_out[r, b, :, ns] = mm(dz, w1[ns, :], NT).astype(BF16)
        sc2.to_partner(r, b).start()
        dz = pre_piece(r, 0, b)
        sc2.to_partner(r, b).wait_recv()
        for ns in columns(width):
            put(ns, mm(dz, w1[ns, :], NT) + p_in[r, b, :, ns].astype(F32))

    def pair_out(r, b):
        dyg.wait_shared(r, b)

        def put(ns, v):
            sums[r - 1, b, :, ns] = v.astype(BF16)
        pair(r, b, put)

    def own_body(b):
        dyg.wait_partner(b)

        def put(ns, v):
            own[b, :, ns] = v
        pair(0, b, put)

    def near_body(b):
        dyg.relay(b)
        loop(2, lambda i: pair_out(R_RIGHT + 2 * i, b))
        sc2.send_near(b)
        recall(2 * b, 2)

    def far_body(b):
        dyg.relay_far(b)
        pair_out(R_FAR, b)
        dyg.drain_far(b)
        sc2.send_far(b)
        h2g.start_own(b)

    def dw1_pair(r, b):
        def body(p):
            dw1[...] += mm(hb[CORES * r + p, b], z[b, place.block(r, p)], TN)
        loop(CORES, body)

    def dw1_own(b):
        h2g.wait_partner(b)
        dw1_pair(0, b)

    def dw1_near(b):
        def body(i):
            r = R_RIGHT + 2 * i
            h2g.wait_shared(r, b)
            dw1_pair(r, b)
        loop(2, body)

    def dw1_far(b):
        h2g.relay_far(b)
        h2g.wait_shared(R_FAR, b)
        dw1_pair(R_FAR, b)
        h2g.drain(b)
        for peer in neighbours:
            pl.semaphore_signal(credit.at[b], inc=1, device_id={'tp': peer}, device_id_type=MESH)
        normalize(xi, hb, gain1_ref, bias1_ref, b)

    def start_h1(b):
        pl.semaphore_wait(credit.at[b], len(neighbours))
        h1g.start_own(b)

    def back2(b):
        sc2.wait_final(b)

        def body(i):
            rs = span(i, STEP)
            grad = sc2.total(own, b, rs)
            x_hat, inv_std = ln_stats(xm[b, rs].astype(F32))
            dyf = tok[0, b, rs].astype(F32)
            dx1 = (dyf + ln_bwd(grad, x_hat, inv_std, gain2_ref[...])).astype(BF16)
            tok[0, b, rs] = dx1
            for k, v in enumerate((grad * x_hat, grad, dx1.astype(F32), dyf)):
                vacc[2 + k] += fold8(v)
        loop(rows // STEP, body)
        mg.start_own(b)

    def last2(b):
        dyg.drain_near(b)
        sc2.send_last(b)

    def attend(r, p, b):
        mid, blk = tok[CORES * r + p, b], place.block(r, p)
        qs = span(blk, rows)
        dwo[...] += mm(ctx_t[b, :, qs], mid, NN)
        dctx = mm(mid, wo[...], NT).astype(BF16)
        dctx_t = turn(dctx)
        qt = q_t[b, :, qs]
        q_h, d_h = split_heads(turn(qt)), split_heads(dctx)
        delta = [jnp.sum(v, axis=-1, keepdims=True) for v in split_heads(dctx.astype(F32) * ctx[b, blk])]
        lse_v = jnp.transpose(lse[b, blk])
        l_col = [lse_v[:, h:h + 1] for h in HEADS]
        last = blk // (TK // rows)
        clear(head_acc)

        def tile(j, masked=False):
            ks = span(j, TK)
            kk, vv = k_t[b, :, ks], v_t[b, :, ks]
            for h in HEADS:
                hs = pl.ds(pl.multiple_of(b * LANES + h * dim, dim), dim)
                top = slice(h * dim, (h + 1) * dim)
                prob = jnp.exp2(mm(q_h[h], kk, NN) * exp_scale - l_col[h])
                if masked:
                    prob = jnp.where(visible(blk, j, rows), prob, 0.0)
                ds = (prob * (mm(d_h[h], vv, NN) - delta[h])).astype(BF16)
                head_acc[h] += mm(ds, kk, NT)
                acc[0, hs, ks] += mm(qt[top], ds, NN)
                acc[1, hs, ks] += mm(dctx_t[top], prob.astype(BF16), NN)

        tile(last, True)
        loop(last, tile)
        dq = jnp.where(first_head(head_acc.shape[1:]), head_acc[0], head_acc[1]) * scale
        dqkv[b, :LANES, qs] = turn(dq)

    def attend_own(i):
        b, p = i // CORES, lax.rem(i, CORES)

        @pl.when(p == 0)
        def _():
            mg.wait_partner(b)
        attend(0, p, b)

    def attend_near(b):
        for r in (R_RIGHT, R_LEFT):
            mg.wait_shared(r, b)

        def body(i):
            @pl.when((i == 2 * CORES - 1) & (b == 0))
            def _():
                mg.relay(1)
                start_h1(0)
            attend(R_RIGHT + 2 * (i // CORES), lax.rem(i, CORES), b)
        loop(2 * CORES, body)

    def partial_rows(r, p, b):
        return turn(dqkv[b, :, span(place.block(r, p), rows)])

    def reduce_out(r, b):
        lhs = partial_rows(r, 0, b)
        sc1.to_partner(r, b).wait_recv()
        for ns in columns(width):
            sums[r - 1, b, :, ns] = (mm(lhs, wqkv[:, ns], NN) + p_in[r, b, :, ns].astype(F32)).astype(BF16)

    def attend_far(b):
        @pl.when(b == 0)
        def _():
            mg.relay_far(0)
        mg.wait_shared(R_FAR, b)
        loop(CORES, lambda p: attend(R_FAR, p, b))

        @pl.when(b == 1)
        def _():
            sc1.send_last(0)
        mine = span(b, LANES)
        dqkv[b, LANES:2 * LANES] = (acc[0, mine] * scale).astype(BF16)
        dqkv[b, 2 * LANES:] = acc[1, mine].astype(BF16)

        def to_partner(i):
            r = lax.rem(R_FAR + i, place.chips)
            lhs = partial_rows(r, 1, b)
            for ns in columns(width):
                p_out[r, b, :, ns] = mm(lhs, wqkv[:, ns], NN).astype(BF16)
            sc1.to_partner(r, b).start()

        loop(place.chips, to_partner)
        reduce_out(R_FAR, b)
        sc1.send_far(b)
        loop(2, lambda i: reduce_out(R_RIGHT + 2 * i, b))
        sc1.send_near(b)
        lhs = partial_rows(0, 0, b)
        sc1.to_partner(0, b).wait_recv()
        for ns in columns(width):
            own[b, :, ns] = mm(lhs, wqkv[:, ns], NN) + p_in[0, b, :, ns].astype(F32)

    def dw_pair(r, b):
        def body(p):
            dwqkv[...] += mm(dqkv[b, :, span(place.block(r, p), rows)], hb[CORES * r + p, b], NN)
        loop(CORES, body)

    def dw_own(b):
        h1g.wait_partner(b)
        dw_pair(0, b)

    def dw_near(b):
        def body(i):
            r = R_RIGHT + 2 * i
            h1g.wait_shared(r, b)
            dw_pair(r, b)
        loop(2, body)

    def dw_far(b):
        h1g.relay_far(b)
        h1g.wait_shared(R_FAR, b)
        dw_pair(R_FAR, b)

    def back1(b):
        sc1.wait_final(b)

        def body(i):
            rs = span(i, STEP)
            grad = sc1.total(own, b, rs)
            x_hat, inv_std = ln_stats(xi[b, rs].astype(F32))
            dx = (tok[0, b, rs].astype(F32) + ln_bwd(grad, x_hat, inv_std, gain1_ref[...])).astype(BF16)
            xi[b, rs] = dx
            for k, v in enumerate((grad * x_hat, grad)):
                vacc[k] += fold8(v)
        loop(rows // STEP, body)

    loop(2, own_body)
    loop(2, near_body)
    loop(2, far_body)
    recall(4, 2 * blocks - 4)
    clear(acc)
    loop(2, last2)
    h2g.relay(0)
    loop(2, dw1_own)
    h2g.relay(1)
    loop(2, dw1_near)
    loop(2, back2)
    stores = start_copies(((dw2, dw2_hbm),), lsem)
    sc2.finish()
    loop(len(BATCH) * CORES, attend_own)
    loop(2, dw1_far)
    stores += start_copies(((dw1, dw1_hbm),), lsem.at[pl.ds(1, 1)])
    db1_ref[...] = jnp.sum(db1[...], axis=0, keepdims=True)
    mg.relay(0)

    def batch(b):
        @pl.when(b == 1)
        def _():
            mg.relay_far(1)
            start_h1(1)
        attend_near(b)
        attend_far(b)

    loop(2, batch)
    h1g.relay(0)
    loop(2, dw_own)
    ones = jnp.ones((SUB, dqkv.shape[2]), BF16)
    dbqkv_ref[...] = (mm(ones, dqkv[0], NT) + mm(ones, dqkv[1], NT))[:1]
    sc1.send_last(1)
    h1g.relay(1)
    loop(2, dw_near)
    loop(2, back1)
    stores += start_copies(((xi, dx_hbm), (dwo, dwo_hbm)), lsem.at[pl.ds(2, 2)])
    for k in range(vacc.shape[0]):
        vsend[k:k + 1] = jnp.sum(vacc[k], axis=0, keepdims=True)
    swap = remote(vsend, vrecv, v_ss.at[0], v_rs.at[n_tp], place.partner)
    swap.start()
    swap.wait_recv()
    vring[place.x] = vsend[...] + vrecv[...]
    ring = [remote(vring.at[place.x], vring.at[place.x], v_ss.at[r], v_rs.at[place.x], peer)
            for r, peer in zip(RING, (place.right, place.far, place.left))]
    for copy in ring:
        copy.start()
    loop(2, dw_far)
    stores += start_copies(((dwqkv, dwqkv_hbm),), lsem.at[pl.ds(4, 1)])
    for r in RING:
        other = lax.rem(place.x + r, place.chips)
        remote(vring.at[other], vring.at[other], v_ss.at[r], v_rs.at[other], place.right).wait_recv()
    vecs_ref[...] = functools.reduce(jnp.add, [vring[k] for k in range(vring.shape[0])])[:vecs_ref.shape[0]]
    swap.wait_send()
    for copy in ring:
        copy.wait_send()
    for b in BATCH:
        dyg.drain_own(b)
        mg.drain(b)
        h1g.drain(b)
    sc1.finish()
    for store in stores:
        store.wait()


def backward(n_tp, scale, d_out, x_mid, z, w1, w2, q_t, k_t, v_t, x_in, wqkv_t, wo, gain2, bias2, gain1, bias1):
    batch, rows, width = d_out.shape
    units = w2.shape[0]
    seq = q_t.shape[2]
    blocks = seq // rows
    qkv_rows = wqkv_t.shape[0]
    any_spec = pl.BlockSpec(memory_space=pl.ANY)
    vm = pl.BlockSpec(memory_space=pltpu.VMEM)
    slots = pltpu.VMEM((SLOT_END, batch, rows, width), BF16)
    row = pltpu.VMEM((SUB, width), F32)

    def shape(*dims):
        return jax.ShapeDtypeStruct(dims, F32)

    return pl.pallas_call(
        functools.partial(backward_kernel, n_tp, scale),
        name='layer_backward',
        out_shape=(jax.ShapeDtypeStruct((batch, rows, width), BF16), shape(width, units), shape(units, width),
                   shape(qkv_rows, width), shape(LANES, width), shape(1, units), shape(1, qkv_rows), shape(6, width)),
        in_specs=[any_spec] * 11 + [vm] * 4,
        out_specs=(*[any_spec] * 5, vm, vm, vm),
        scratch_shapes=[
            slots, slots, *scatter_scratch(rows, width),
            pltpu.VMEM((batch, blocks, rows, units), BF16),
            pltpu.VMEM((width, units), BF16), pltpu.VMEM((units, width), BF16),
            pltpu.VMEM((width, units), F32), pltpu.VMEM((units, width), F32),
            pltpu.VMEM((batch, rows, width), F32), *[pltpu.VMEM((batch, rows, width), BF16)] * 2,
            pltpu.VMEM((SUB, units), F32), *[pltpu.VMEM((batch, LANES, seq), BF16)] * 4,
            pltpu.VMEM((batch, blocks, rows, LANES), F32), pltpu.VMEM((batch, blocks, SUB, rows), F32),
            pltpu.VMEM((len(HEADS), rows, seq), F32), pltpu.VMEM((len(HEADS), rows, LANES), F32),
            pltpu.VMEM((qkv_rows, width), BF16), pltpu.VMEM((LANES, width), BF16), pltpu.VMEM((batch, qkv_rows, seq), BF16),
            pltpu.VMEM((qkv_rows, width), F32), pltpu.VMEM((LANES, width), F32),
            pltpu.VMEM((6, SUB, width), F32), row, row, pltpu.VMEM((n_tp // CORES, SUB, width), F32),
            *copy_sems(*[SLOT_END, SLOT_END + 1] * 4, *[10] * 4),
            pltpu.SemaphoreType.DMA((11,)), pltpu.SemaphoreType.DMA((4,)), pltpu.SemaphoreType.DMA((n_tp + 1,)),
            pltpu.SemaphoreType.REGULAR((batch,)),
        ],
        compiler_params=pltpu.CompilerParams(collective_id=1, has_side_effects=True, vmem_limit_bytes=VMEM_LIMIT),
    )(d_out, x_mid, z.reshape(batch, blocks, rows, units), w1, w2, q_t, k_t, v_t, x_in, wqkv_t, wo,
      *[v.reshape(1, width) for v in (gain2, bias2, gain1, bias1)])


def place_results(big, small):
    pieces = 4

    def kernel(*refs):
        count, rest = len(big), len(small)
        src, small_in = refs[:count], refs[count:count + rest]
        dst, small_out = refs[count + rest:2 * count + rest], refs[2 * count + rest:2 * (count + rest)]
        bufs, sem_in, sem_out = refs[2 * (count + rest):-2], refs[-2], refs[-1]
        moves = []
        for i, buf in enumerate(bufs):
            step = buf.shape[0] // pieces
            for j in range(pieces):
                rs = pl.ds(j * step, step)
                moves.append((pltpu.make_async_copy(src[i].at[rs], buf.at[rs], sem_in.at[i, j]),
                              pltpu.make_async_copy(buf.at[rs], dst[i].at[rs], sem_out.at[i, j])))
        for fetch, _ in moves:
            fetch.start()
        for ref_in, ref_out in zip(small_in, small_out):
            ref_out[...] = ref_in[...]
        for fetch, put in moves:
            fetch.wait()
            put.start()
        for _, put in moves:
            put.wait()

    any_spec = pl.BlockSpec(memory_space=pl.ANY)
    vm = pl.BlockSpec(memory_space=pltpu.VMEM)
    return pl.pallas_call(
        kernel,
        name='place_results',
        out_shape=[jax.ShapeDtypeStruct(v.shape, v.dtype) for v in (*big, *small)],
        in_specs=[any_spec] * len(big) + [vm] * len(small),
        out_specs=[any_spec] * len(big) + [vm] * len(small),
        scratch_shapes=[pltpu.VMEM(v.shape, v.dtype) for v in big] + [pltpu.SemaphoreType.DMA((len(big), pieces))] * 2,
        compiler_params=pltpu.CompilerParams(vmem_limit_bytes=VMEM_LIMIT),
    )(*big, *small)


def solution(mesh):
    n_tp = mesh.shape['tp']

    def local_backward(x_in, x_mid, d_out, q_saved, k_saved, v_saved, z_saved, ln1_gain, ln1_bias, ln2_gain, ln2_bias, w_qkv, w_proj, w_fc1, w_fc2):
        batch, seq, heads, dim = q_saved.shape
        width = x_in.shape[-1]
        scale = dim ** -0.5

        def feature_rows(a):
            return jnp.transpose(a, (0, 2, 3, 1)).reshape(batch, heads * dim, seq)

        q_t, k_t, v_t = feature_rows(q_saved), feature_rows(k_saved), feature_rows(v_saved)
        wqkv_t = jnp.transpose(w_qkv, (0, 2, 3, 1)).reshape(w_qkv.shape[0] * heads * dim, width)
        wo = w_proj.reshape(heads * dim, width)
        grad_x, grad_wfc1, grad_wfc2, dwqkv, dwo, db1, dbqkv, grad_vecs = backward(
            n_tp, scale, d_out, x_mid, z_saved, w_fc1, w_fc2, q_t, k_t, v_t, x_in, wqkv_t, wo,
            ln2_gain, ln2_bias, ln1_gain, ln1_bias)
        grad_x, grad_wfc1, grad_wfc2, dwqkv, dwo, db1, dbqkv, grad_vecs = place_results(
            (grad_x.reshape(batch * x_in.shape[1], width), grad_wfc1, grad_wfc2, dwqkv, dwo), (db1, dbqkv, grad_vecs))
        grad_x = grad_x.reshape(x_in.shape)
        grad_wqkv = jnp.transpose(dwqkv.reshape(-1, heads, dim, width), (0, 3, 1, 2))
        grad_bqkv = dbqkv.reshape(-1, heads, dim)
        grad_wproj = dwo.reshape(heads, dim, width)
        return grad_x, grad_wqkv, grad_bqkv, grad_wproj, grad_wfc1, db1.reshape(-1), grad_wfc2, grad_vecs

    tok_spec = P('dp', 'tp', None)
    head_spec = P('dp', None, 'tp', None)
    in_specs = (tok_spec, tok_spec, tok_spec, head_spec, head_spec, head_spec, P('dp', None, 'tp'),
                P(None), P(None), P(None), P(None),
                P(None, None, 'tp', None), P('tp', None, None), P(None, 'tp'), P('tp', None))
    out_specs = (tok_spec, P('dp', None, 'tp', None), P('dp', 'tp', None), P(('dp', 'tp'), None, None),
                 P('dp', 'tp'), P(('dp', 'tp')), P(('dp', 'tp'), None), P('dp', None))
    return jax.shard_map(local_backward, mesh=mesh, in_specs=in_specs, out_specs=out_specs, check_vma=False)
```

```python
import functools

import jax
import jax.numpy as jnp
from jax import lax
from jax.experimental import pallas as pl
from jax.experimental.pallas import tpu as pltpu
from jax.sharding import PartitionSpec as P

LN_EPS = 1e-5
GELU_COEF = 0.044715
GELU_SCALE = 0.7978845608028654
LOG2E = 1.4426950408889634
MESH = pl.DeviceIdType.MESH
F32 = jnp.float32
BF16 = jnp.bfloat16
VMEM_LIMIT = 227 << 18

NN = (((1,), (0,)), ((), ()))
NT = (((1,), (1,)), ((), ()))
TN = (((0,), (0,)), ((), ()))

CORES = 2
BATCH = range(2)
HEADS = range(2)
RING = R_RIGHT, R_FAR, R_LEFT = 1, 2, 3
SLOT_P, SLOT_R, SLOT_F, SLOT_L, SLOT_END = 1, 2, 4, 6, 8
PARTNER, RIGHT, LEFT, FWD_R, FWD_L = range(5)
NEAR_R, NEAR_L, FAR_R, FAR_L, LAST_R, LAST_L = range(4, 10)
SUB = 8
LANES = 128
TK = 512
NC = 256
STEP = 64


def mm(a, b, dims):
    return lax.dot_general(a, b, dims, preferred_element_type=F32)


def loop(count, body):
    def run(i, carry):
        body(i)
        return carry
    lax.fori_loop(0, count, run, 0)


def fold8(v):
    return jnp.sum(v.reshape(v.shape[0] // SUB, SUB, v.shape[1]), axis=0)


def turn(v):
    return jnp.transpose(v.astype(F32)).astype(BF16)


def span(i, size):
    return pl.ds(pl.multiple_of(i * size, size), size)


def columns(width):
    return [pl.ds(n * NC, NC) for n in range(width // NC)]


def clear(*refs):
    for ref in refs:
        ref[...] = jnp.zeros_like(ref)


def ln_stats(rows):
    centered = rows - jnp.mean(rows, axis=-1, keepdims=True)
    inv_std = lax.rsqrt(jnp.mean(centered * centered, axis=-1, keepdims=True) + LN_EPS)
    return centered * inv_std, inv_std


def ln_bwd(grad, x_hat, inv_std, gain):
    grad_hat = grad * gain
    centered = grad_hat - jnp.mean(grad_hat, axis=-1, keepdims=True)
    return inv_std * (centered - x_hat * jnp.mean(grad_hat * x_hat, axis=-1, keepdims=True))


def normalize(src, dst, gain, bias, b):
    def body(i):
        rs = span(i, STEP)
        x_hat, _ = ln_stats(src[b, rs].astype(F32))
        dst[0, b, rs] = (x_hat * gain[...] + bias[...]).astype(BF16)

    loop(src.shape[1] // STEP, body)


def start_copies(pairs, sems):
    copies = [pltpu.make_async_copy(s, d, sems.at[i]) for i, (s, d) in enumerate(pairs)]
    for copy in copies:
        copy.start()
    return copies


class Place:
    def __init__(self, n_tp):
        self.chips = n_tp // CORES
        me = lax.axis_index('tp')
        self.x = me // CORES
        self.c = lax.rem(me, CORES)
        self.partner = self.block(0, 1)
        self.right, self.far, self.left = [self.block(r, 0) for r in RING]

    def block(self, r, p):
        return lax.rem(self.x + r, self.chips) * CORES + lax.rem(self.c + p, CORES)

    def enter(self, peers):
        barrier = pltpu.get_barrier_semaphore()
        for peer in peers:
            pl.semaphore_signal(barrier, inc=1, device_id={'tp': peer}, device_id_type=MESH)
        pl.semaphore_wait(barrier, len(peers))


def remote(src, dst, ssem, rsem, peer):
    return pltpu.make_async_remote_copy(src_ref=src, dst_ref=dst, send_sem=ssem, recv_sem=rsem,
                                        device_id={'tp': peer}, device_id_type=MESH)


class Gather:
    def __init__(self, place, own, buf, ssem, rsem):
        self.place, self.own, self.buf, self.ssem, self.rsem = place, own, buf, ssem, rsem
        half = buf.shape[-2] // 2
        self.lo, self.hi = pl.ds(0, half), pl.ds(half, half)

    def _own(self, kind, slot, b, peer):
        return remote(self.own.at[b], self.buf.at[slot, b], self.ssem.at[kind, b], self.rsem.at[slot, b], peer)

    def to_partner(self, b):
        return self._own(PARTNER, SLOT_P, b, self.place.partner)

    def to_right(self, b):
        return self._own(RIGHT, SLOT_L, b, self.place.right)

    def to_left(self, b):
        return self._own(LEFT, SLOT_R, b, self.place.left)

    def fwd_right(self, b):
        return remote(self.buf.at[SLOT_L, b, self.lo], self.buf.at[SLOT_F, b, self.lo],
                      self.ssem.at[FWD_R, b], self.rsem.at[SLOT_F, b], self.place.right)

    def fwd_left(self, b):
        return remote(self.buf.at[SLOT_R, b, self.hi], self.buf.at[SLOT_F, b, self.hi],
                      self.ssem.at[FWD_L, b], self.rsem.at[SLOT_END, b], self.place.left)

    def share(self, r, b):
        slot = CORES * r
        return remote(self.buf.at[slot, b], self.buf.at[slot + 1, b], self.ssem.at[FWD_L + r, b], self.rsem.at[slot + 1, b],
                      self.place.partner)

    def start_own(self, b):
        self.to_right(b).start()
        self.to_left(b).start()
        self.to_partner(b).start()

    def relay(self, b):
        self.to_right(b).wait_recv()
        self.fwd_right(b).start()
        self.to_left(b).wait_recv()
        self.fwd_left(b).start()
        self.share(R_LEFT, b).start()
        self.share(R_RIGHT, b).start()

    def relay_far(self, b):
        self.fwd_right(b).wait_recv()
        self.fwd_left(b).wait_recv()
        self.share(R_FAR, b).start()

    def wait_shared(self, r, b):
        self.share(r, b).wait_recv()

    def wait_partner(self, b):
        self.to_partner(b).wait_recv()

    def drain_own(self, b):
        for copy in (self.to_partner, self.to_right, self.to_left):
            copy(b).wait_send()

    def drain_near(self, b):
        for copy in (self.fwd_right(b), self.fwd_left(b), self.share(R_RIGHT, b), self.share(R_LEFT, b)):
            copy.wait_send()

    def drain_far(self, b):
        self.share(R_FAR, b).wait_send()

    def drain(self, b):
        self.drain_own(b)
        self.drain_near(b)
        self.drain_far(b)


class Scatter:
    def __init__(self, place, p_out, p_in, sums, fin, transit, ssem, rsem):
        self.place = place
        self.p_out, self.p_in, self.sums, self.fin, self.transit = p_out, p_in, sums, fin, transit
        self.ssem, self.rsem = ssem, rsem
        half = sums.shape[-2] // 2
        self.lo, self.hi = pl.ds(0, half), pl.ds(half, half)

    def to_partner(self, r, b):
        return remote(self.p_out.at[r, b], self.p_in.at[r, b], self.ssem.at[r, b], self.rsem.at[r, b], self.place.partner)

    def _hop(self, kind, src, dst, b, peer):
        return remote(src, dst, self.ssem.at[kind, b], self.rsem.at[kind, b], peer)

    def near_right(self, b):
        return self._hop(NEAR_R, self.sums.at[0, b, self.hi], self.fin.at[0, b, self.hi], b, self.place.right)

    def near_left(self, b):
        return self._hop(NEAR_L, self.sums.at[2, b, self.lo], self.fin.at[1, b, self.lo], b, self.place.left)

    def far_right(self, b):
        return self._hop(FAR_R, self.sums.at[1, b, self.lo], self.transit.at[0, b], b, self.place.right)

    def far_left(self, b):
        return self._hop(FAR_L, self.sums.at[1, b, self.hi], self.transit.at[1, b], b, self.place.left)

    def last_right(self, b):
        return self._hop(LAST_R, self.sums.at[0, b, self.lo], self.fin.at[0, b, self.lo], b, self.place.right)

    def last_left(self, b):
        return self._hop(LAST_L, self.sums.at[2, b, self.hi], self.fin.at[1, b, self.hi], b, self.place.left)

    def send_near(self, b):
        self.near_right(b).start()
        self.near_left(b).start()

    def send_far(self, b):
        self.far_right(b).start()
        self.far_left(b).start()

    def send_last(self, b):
        for arrived, slot, lane, rows, onward in ((self.far_right, 0, 0, self.lo, self.last_right),
                                                  (self.far_left, 2, 1, self.hi, self.last_left)):
            arrived(b).wait_recv()
            self.sums[slot, b, rows] = (self.sums[slot, b, rows].astype(F32) + self.transit[lane, b].astype(F32)).astype(BF16)
            onward(b).start()

    def wait_final(self, b):
        for copy in (self.near_right, self.near_left, self.last_right, self.last_left):
            copy(b).wait_recv()

    def total(self, own, b, rs):
        return own[b, rs] + self.fin[0, b, rs].astype(F32) + self.fin[1, b, rs].astype(F32)

    def finish(self):
        for b in BATCH:
            for r in (0, *RING):
                self.to_partner(r, b).wait_send()
            for copy in (self.near_right, self.near_left, self.far_right, self.far_left, self.last_right, self.last_left):
                copy(b).wait_send()


def scatter_scratch(rows, width):
    def buf(*lead):
        return pltpu.VMEM((*lead, len(BATCH), rows, width), BF16)
    return [buf(4), buf(4), buf(3), buf(2), pltpu.VMEM((2, len(BATCH), rows // 2, width), BF16)]


def copy_sems(*counts):
    return [pltpu.SemaphoreType.DMA((count, len(BATCH))) for count in counts]


def first_head(shape):
    return lax.broadcasted_iota(jnp.int32, shape, 1) < shape[1] // len(HEADS)


def split_heads(v):
    first, zero = first_head(v.shape), jnp.zeros_like(v)
    return [jnp.where(first, v, zero), jnp.where(first, zero, v)]


def visible(blk, j, rows):
    row_id = blk * rows + lax.broadcasted_iota(jnp.int32, (rows, TK), 0)
    return row_id >= j * TK + lax.broadcasted_iota(jnp.int32, (rows, TK), 1)


def attn_fwd_block(b, blk, q_t, k_t, v_t, ctx_t, ctx, lse, s_buf, m_buf, scale):
    rows = ctx.shape[2]
    qs = span(blk, rows)
    last = blk // (TK // rows)
    q_h = split_heads(turn(q_t[b, :, qs]))

    def fold(f, v):
        parts = [v[:, i:i + LANES] for i in range(0, TK, LANES)]
        return functools.reduce(f, parts)

    def score(j, masked=False):
        kk = k_t[b, :, span(j, TK)]
        for h in HEADS:
            s = mm(q_h[h], kk, NN) * scale
            if masked:
                s = jnp.where(visible(blk, j, rows), s, -1e30)
            s_buf[h, :, span(j, TK)] = s
            top = fold(jnp.maximum, s)
            m_buf[h] = top if masked else jnp.maximum(m_buf[h], top)

    score(last, True)
    loop(last, score)
    m_col = [jnp.max(m_buf[h], axis=-1, keepdims=True) for h in HEADS]
    clear(m_buf)

    def total(j):
        for h in HEADS:
            m_buf[h] += fold(jnp.add, jnp.exp2(s_buf[h, :, span(j, TK)] - m_col[h]))

    loop(last + 1, total)
    l_col = [m_col[h] + jnp.log2(jnp.sum(m_buf[h], axis=-1, keepdims=True)) for h in HEADS]
    clear(m_buf)

    def weigh(j):
        vv = v_t[b, :, span(j, TK)]
        for h in HEADS:
            m_buf[h] += mm(jnp.exp2(s_buf[h, :, span(j, TK)] - l_col[h]).astype(BF16), vv, NT)

    loop(last + 1, weigh)
    first = first_head(m_buf.shape[1:])
    out = jnp.where(first, m_buf[0], m_buf[1])
    ctx[b, blk] = out
    lse_t = jnp.transpose(jnp.where(first, *l_col))
    for h in HEADS:
        top = h * (LANES // len(HEADS))
        lse[b, blk, h:h + 1] = lse_t[top:top + 1]
    ctx_t[b, :, qs] = turn(out)


def backward_kernel(n_tp, scale, dy_hbm, xm_hbm, z_hbm, w1_hbm, w2_hbm, q_hbm, k_hbm, v_hbm, xi_hbm, wqkv_hbm, wo_hbm,
                    gain2_ref, bias2_ref, gain1_ref, bias1_ref,
                    xi, dw1, dw2, dwqkv, dwo, db1_ref, dbqkv_ref, vecs_ref,
                    tok, hb, p_out, p_in, sums, fin, transit,
                    z, w1, w2, own, xm, db1, q_t, k_t, v_t, ctx_t, ctx, lse, acc, head_acc,
                    wqkv, wo, dqkv, vacc, vsend, vrecv,
                    dy_ss, dy_rs, h2_ss, h2_rs, dx_ss, dx_rs, h1_ss, h1_rs, rs2_ss, rs2_rs, rs1_ss, rs1_rs,
                    lsem, v_ss, v_rs, credit):
    place = Place(n_tp)
    rows, width = dy_hbm.shape[1:]
    units = w2.shape[0]
    blocks = ctx.shape[1]
    neighbours = (place.partner, place.right, place.left)
    place.enter((*neighbours, place.far))
    dyg = Gather(place, dy_hbm, tok, dy_ss, dy_rs)
    mg = Gather(place, tok.at[0], tok, dx_ss, dx_rs)
    h2g = Gather(place, hb.at[0], hb, h2_ss, h2_rs)
    h1g = Gather(place, hb.at[0], hb, h1_ss, h1_rs)
    sc2 = Scatter(place, p_out, p_in, sums, fin, transit, rs2_ss, rs2_rs)
    sc1 = Scatter(place, p_out, p_in, sums, fin, transit, rs1_ss, rs1_rs)
    for b in BATCH:
        dyg.start_own(b)
    loads = start_copies(((xm_hbm, xm), (dy_hbm, tok.at[0]), (w2_hbm, w2), (z_hbm, z), (w1_hbm, w1),
                          (q_hbm, q_t), (k_hbm, k_t), (v_hbm, v_t), (wo_hbm, wo), (wqkv_hbm, wqkv), (xi_hbm, xi)), lsem)
    clear(dw1, dw2, db1, vacc, vsend, dwqkv, dwo, lse)
    loads[0].wait()
    loop(2, functools.partial(normalize, xm, hb, gain2_ref, bias2_ref))
    for load in loads[1:]:
        load.wait()
    exp_scale = scale * LOG2E
    dim = LANES // len(HEADS)

    def recall(lo, count):
        def body(i):
            i = lo + i
            attn_fwd_block(i // blocks, lax.rem(i, blocks), q_t, k_t, v_t, ctx_t, ctx, lse, acc, head_acc, exp_scale)
        loop(count, body)

    def pre_piece(r, p, b):
        dy, blk = tok[CORES * r + p, b], place.block(r, p)
        for fs in columns(units):
            act = mm(dy, w2[fs, :], NT)
            zf = z[b, blk, :, fs].astype(F32)
            t = jnp.tanh(GELU_SCALE * (zf + GELU_COEF * zf * zf * zf))
            half_t = 0.5 * (1.0 + t)
            slope = half_t + 0.5 * zf * (1.0 - t * t) * GELU_SCALE * (1.0 + 3.0 * GELU_COEF * zf * zf)
            u = (zf * half_t).astype(BF16)
            dzv = (act * slope).astype(BF16)
            z[b, blk, :, fs] = dzv
            db1[:, fs] += fold8(dzv.astype(F32))
            dw2[fs, :] += mm(u, dy, TN)
        return z[b, blk]

    def pair(r, b, put):
        dz = pre_piece(r, 1, b)
        for ns in columns(width):
            p_out[r, b, :, ns] = mm(dz, w1[ns, :], NT).astype(BF16)
        sc2.to_partner(r, b).start()
        dz = pre_piece(r, 0, b)
        sc2.to_partner(r, b).wait_recv()
        for ns in columns(width):
            put(ns, mm(dz, w1[ns, :], NT) + p_in[r, b, :, ns].astype(F32))

    def pair_out(r, b):
        dyg.wait_shared(r, b)

        def put(ns, v):
            sums[r - 1, b, :, ns] = v.astype(BF16)
        pair(r, b, put)

    def own_body(b):
        dyg.wait_partner(b)

        def put(ns, v):
            own[b, :, ns] = v
        pair(0, b, put)

    def near_body(b):
        dyg.relay(b)
        loop(2, lambda i: pair_out(R_RIGHT + 2 * i, b))
        sc2.send_near(b)
        recall(2 * b, 2)

    def far_body(b):
        dyg.relay_far(b)
        pair_out(R_FAR, b)
        dyg.drain_far(b)
        sc2.send_far(b)
        h2g.start_own(b)

    def dw1_pair(r, b):
        def body(p):
            dz = z[b, place.block(r, p)]
            for ns in columns(width):
                dw1[ns, :] += mm(hb[CORES * r + p, b, :, ns], dz, TN)
        loop(CORES, body)

    def dw1_own(b):
        h2g.wait_partner(b)
        dw1_pair(0, b)

    def dw1_near(b):
        def body(i):
            r = R_RIGHT + 2 * i
            h2g.wait_shared(r, b)
            dw1_pair(r, b)
        loop(2, body)

    def dw1_far(b):
        h2g.relay_far(b)
        h2g.wait_shared(R_FAR, b)
        dw1_pair(R_FAR, b)
        h2g.drain(b)
        for peer in neighbours:
            pl.semaphore_signal(credit.at[b], inc=1, device_id={'tp': peer}, device_id_type=MESH)
        normalize(xi, hb, gain1_ref, bias1_ref, b)

    def start_h1(b):
        pl.semaphore_wait(credit.at[b], len(neighbours))
        h1g.start_own(b)

    def back2(b):
        sc2.wait_final(b)

        def body(i):
            rs = span(i, STEP)
            grad = sc2.total(own, b, rs)
            x_hat, inv_std = ln_stats(xm[b, rs].astype(F32))
            dyf = tok[0, b, rs].astype(F32)
            dx1 = (dyf + ln_bwd(grad, x_hat, inv_std, gain2_ref[...])).astype(BF16)
            tok[0, b, rs] = dx1
            for k, v in enumerate((grad * x_hat, grad, dx1.astype(F32), dyf)):
                vacc[2 + k] += fold8(v)
        loop(rows // STEP, body)
        mg.start_own(b)

    def last2(b):
        dyg.drain_near(b)
        sc2.send_last(b)

    def attend(r, p, b):
        mid, blk = tok[CORES * r + p, b], place.block(r, p)
        qs = span(blk, rows)
        dwo[...] += mm(ctx_t[b, :, qs], mid, NN)
        dctx = mm(mid, wo[...], NT).astype(BF16)
        dctx_t = turn(dctx)
        qt = q_t[b, :, qs]
        q_h, d_h = split_heads(turn(qt)), split_heads(dctx)
        delta = [jnp.sum(v, axis=-1, keepdims=True) for v in split_heads(dctx.astype(F32) * ctx[b, blk])]
        lse_v = jnp.transpose(lse[b, blk])
        l_col = [lse_v[:, h:h + 1] for h in HEADS]
        last = blk // (TK // rows)
        clear(head_acc)

        def tile(j, masked=False):
            ks = span(j, TK)
            kk, vv = k_t[b, :, ks], v_t[b, :, ks]
            for h in HEADS:
                hs = pl.ds(pl.multiple_of(b * LANES + h * dim, dim), dim)
                top = slice(h * dim, (h + 1) * dim)
                prob = jnp.exp2(mm(q_h[h], kk, NN) * exp_scale - l_col[h])
                if masked:
                    prob = jnp.where(visible(blk, j, rows), prob, 0.0)
                ds = (prob * (mm(d_h[h], vv, NN) - delta[h])).astype(BF16)
                head_acc[h] += mm(ds, kk, NT)
                acc[0, hs, ks] += mm(qt[top], ds, NN)
                acc[1, hs, ks] += mm(dctx_t[top], prob.astype(BF16), NN)

        tile(last, True)
        loop(last, tile)
        dq = jnp.where(first_head(head_acc.shape[1:]), head_acc[0], head_acc[1]) * scale
        dqkv[b, :LANES, qs] = turn(dq)

    def attend_own(i):
        b, p = i // CORES, lax.rem(i, CORES)

        @pl.when(p == 0)
        def _():
            mg.wait_partner(b)
        attend(0, p, b)

    def attend_near(b):
        for r in (R_RIGHT, R_LEFT):
            mg.wait_shared(r, b)

        def body(i):
            @pl.when((i == 2 * CORES - 1) & (b == 0))
            def _():
                mg.relay(1)
                start_h1(0)
            attend(R_RIGHT + 2 * (i // CORES), lax.rem(i, CORES), b)
        loop(2 * CORES, body)

    def partial_rows(r, p, b):
        return turn(dqkv[b, :, span(place.block(r, p), rows)])

    def reduce_out(r, b):
        lhs = partial_rows(r, 0, b)
        sc1.to_partner(r, b).wait_recv()
        for ns in columns(width):
            sums[r - 1, b, :, ns] = (mm(lhs, wqkv[:, ns], NN) + p_in[r, b, :, ns].astype(F32)).astype(BF16)

    def attend_far(b):
        @pl.when(b == 0)
        def _():
            mg.relay_far(0)
        mg.wait_shared(R_FAR, b)
        loop(CORES, lambda p: attend(R_FAR, p, b))

        @pl.when(b == 1)
        def _():
            sc1.send_last(0)
        mine = span(b, LANES)
        dqkv[b, LANES:2 * LANES] = (acc[0, mine] * scale).astype(BF16)
        dqkv[b, 2 * LANES:] = acc[1, mine].astype(BF16)

        def to_partner(i):
            r = lax.rem(R_FAR + i, place.chips)
            lhs = partial_rows(r, 1, b)
            for ns in columns(width):
                p_out[r, b, :, ns] = mm(lhs, wqkv[:, ns], NN).astype(BF16)
            sc1.to_partner(r, b).start()

        loop(place.chips, to_partner)
        reduce_out(R_FAR, b)
        sc1.send_far(b)
        loop(2, lambda i: reduce_out(R_RIGHT + 2 * i, b))
        sc1.send_near(b)
        lhs = partial_rows(0, 0, b)
        sc1.to_partner(0, b).wait_recv()
        for ns in columns(width):
            own[b, :, ns] = mm(lhs, wqkv[:, ns], NN) + p_in[0, b, :, ns].astype(F32)

    def dw_pair(r, b):
        def body(p):
            part = dqkv[b, :, span(place.block(r, p), rows)]
            for ns in columns(width):
                dwqkv[:, ns] += mm(part, hb[CORES * r + p, b, :, ns], NN)
        loop(CORES, body)

    def dw_own(b):
        h1g.wait_partner(b)
        dw_pair(0, b)

    def dw_near(b):
        def body(i):
            r = R_RIGHT + 2 * i
            h1g.wait_shared(r, b)
            dw_pair(r, b)
        loop(2, body)

    def dw_far(b):
        h1g.relay_far(b)
        h1g.wait_shared(R_FAR, b)
        dw_pair(R_FAR, b)

    def back1(b):
        sc1.wait_final(b)

        def body(i):
            rs = span(i, STEP)
            grad = sc1.total(own, b, rs)
            x_hat, inv_std = ln_stats(xi[b, rs].astype(F32))
            dx = (tok[0, b, rs].astype(F32) + ln_bwd(grad, x_hat, inv_std, gain1_ref[...])).astype(BF16)
            xi[b, rs] = dx
            for k, v in enumerate((grad * x_hat, grad)):
                vacc[k] += fold8(v)
        loop(rows // STEP, body)

    loop(2, own_body)
    loop(2, near_body)
    loop(2, far_body)
    tail = 3
    recall(4, 2 * blocks - 4 - tail)
    loop(2, last2)
    recall(2 * blocks - tail, tail)
    clear(acc)
    h2g.relay(0)
    loop(2, dw1_own)
    h2g.relay(1)
    loop(2, dw1_near)
    loop(2, back2)
    sc2.finish()
    loop(len(BATCH) * CORES, attend_own)
    loop(2, dw1_far)
    db1_ref[...] = jnp.sum(db1[...], axis=0, keepdims=True)
    mg.relay(0)

    def batch(b):
        @pl.when(b == 1)
        def _():
            mg.relay_far(1)
            start_h1(1)
        attend_near(b)
        attend_far(b)

    loop(2, batch)
    h1g.relay(0)
    loop(2, dw_own)
    ones = jnp.ones((SUB, dqkv.shape[2]), BF16)
    dbqkv_ref[...] = (mm(ones, dqkv[0], NT) + mm(ones, dqkv[1], NT))[:1]
    sc1.send_last(1)
    h1g.relay(1)
    loop(2, dw_near)
    loop(2, back1)
    for k in range(vacc.shape[0]):
        vsend[k:k + 1] = jnp.sum(vacc[k], axis=0, keepdims=True)
    swap = remote(vsend, vrecv, v_ss.at[0], v_rs.at[n_tp], place.partner)
    swap.start()
    swap.wait_recv()

    def vring(chip):
        return acc.at[0, span(chip, SUB), pl.ds(0, width)]

    vring(place.x)[...] = vsend[...] + vrecv[...]
    ring = [remote(vring(place.x), vring(place.x), v_ss.at[r], v_rs.at[place.x], peer)
            for r, peer in zip(RING, (place.right, place.far, place.left))]
    for copy in ring:
        copy.start()
    loop(2, dw_far)
    for r in RING:
        other = lax.rem(place.x + r, place.chips)
        remote(vring(other), vring(other), v_ss.at[r], v_rs.at[other], place.right).wait_recv()
    vecs_ref[...] = functools.reduce(jnp.add, [vring(k)[...] for k in range(place.chips)])[:vecs_ref.shape[0]]
    swap.wait_send()
    for copy in ring:
        copy.wait_send()
    for b in BATCH:
        dyg.drain_own(b)
        mg.drain(b)
        h1g.drain(b)
    sc1.finish()


def backward(n_tp, scale, d_out, x_mid, z, w1, w2, q_t, k_t, v_t, x_in, wqkv_t, wo, gain2, bias2, gain1, bias1):
    batch, rows, width = d_out.shape
    units = w2.shape[0]
    seq = q_t.shape[2]
    blocks = seq // rows
    qkv_rows = wqkv_t.shape[0]
    any_spec = pl.BlockSpec(memory_space=pl.ANY)
    vm = pl.BlockSpec(memory_space=pltpu.VMEM)
    slots = pltpu.VMEM((SLOT_END, batch, rows, width), BF16)
    row = pltpu.VMEM((SUB, width), F32)

    return pl.pallas_call(
        functools.partial(backward_kernel, n_tp, scale),
        name='layer_backward',
        out_shape=(pltpu.VMEM((batch, rows, width), BF16), pltpu.VMEM((width, units), F32), pltpu.VMEM((units, width), F32),
                   pltpu.VMEM((qkv_rows, width), F32), pltpu.VMEM((LANES, width), F32),
                   pltpu.VMEM((1, units), F32), pltpu.VMEM((1, qkv_rows), F32), pltpu.VMEM((6, width), F32)),
        in_specs=[any_spec] * 11 + [vm] * 4,
        out_specs=(vm,) * 8,
        scratch_shapes=[
            slots, slots, *scatter_scratch(rows, width),
            pltpu.VMEM((batch, blocks, rows, units), BF16),
            pltpu.VMEM((width, units), BF16), pltpu.VMEM((units, width), BF16),
            pltpu.VMEM((batch, rows, width), F32), pltpu.VMEM((batch, rows, width), BF16),
            pltpu.VMEM((SUB, units), F32), *[pltpu.VMEM((batch, LANES, seq), BF16)] * 4,
            pltpu.VMEM((batch, blocks, rows, LANES), F32), pltpu.VMEM((batch, blocks, SUB, rows), F32),
            pltpu.VMEM((len(HEADS), rows, seq), F32), pltpu.VMEM((len(HEADS), rows, LANES), F32),
            pltpu.VMEM((qkv_rows, width), BF16), pltpu.VMEM((LANES, width), BF16), pltpu.VMEM((batch, qkv_rows, seq), BF16),
            pltpu.VMEM((6, SUB, width), F32), row, row,
            *copy_sems(*[SLOT_END, SLOT_END + 1] * 4, *[10] * 4),
            pltpu.SemaphoreType.DMA((11,)), pltpu.SemaphoreType.DMA((4,)), pltpu.SemaphoreType.DMA((n_tp + 1,)),
            pltpu.SemaphoreType.REGULAR((batch,)),
        ],
        compiler_params=pltpu.CompilerParams(collective_id=1, has_side_effects=True, vmem_limit_bytes=VMEM_LIMIT),
    )(d_out, x_mid, z.reshape(batch, blocks, rows, units), w1, w2, q_t, k_t, v_t, x_in, wqkv_t, wo,
      *[v.reshape(1, width) for v in (gain2, bias2, gain1, bias1)])


def place_results(big, db1, dbqkv, vecs, bias_shape):
    count = len(big)

    def kernel(*refs):
        src, (db1_in, dbqkv_in, vecs_in) = refs[:count], refs[count:count + 3]
        dst, (db1_out, dbqkv_out, vecs_out), sems = refs[count + 3:-4], refs[-4:-1], refs[-1]
        moves = start_copies(zip(src, dst), sems)
        db1_out[...] = db1_in[...]
        vecs_out[...] = vecs_in[...]
        kinds, heads, dim = bias_shape
        for i in range(kinds):
            for h in range(heads):
                start = (i * heads + h) * dim
                dbqkv_out[i, h:h + 1] = dbqkv_in[:, start:start + dim]
        for move in moves:
            move.wait()

    any_spec = pl.BlockSpec(memory_space=pl.ANY)
    vm = pl.BlockSpec(memory_space=pltpu.VMEM)
    return pl.pallas_call(
        kernel,
        name='place_results',
        out_shape=[jax.ShapeDtypeStruct(v.shape, v.dtype) for v in (*big, db1)]
        + [jax.ShapeDtypeStruct(bias_shape, F32), jax.ShapeDtypeStruct(vecs.shape, F32)],
        in_specs=[vm] * (count + 3),
        out_specs=[any_spec] * count + [vm] * 3,
        scratch_shapes=[pltpu.SemaphoreType.DMA((count,))],
        compiler_params=pltpu.CompilerParams(vmem_limit_bytes=8 << 20),
    )(*[pltpu.with_memory_space_constraint(v, pltpu.VMEM) for v in (*big, db1, dbqkv, vecs)])


def solution(mesh):
    n_tp = mesh.shape['tp']

    def local_backward(x_in, x_mid, d_out, q_saved, k_saved, v_saved, z_saved, ln1_gain, ln1_bias, ln2_gain, ln2_bias, w_qkv, w_proj, w_fc1, w_fc2):
        batch, seq, heads, dim = q_saved.shape
        width = x_in.shape[-1]
        scale = dim ** -0.5

        def feature_rows(a):
            return jnp.transpose(a, (0, 2, 3, 1)).reshape(batch, heads * dim, seq)

        q_t, k_t, v_t = feature_rows(q_saved), feature_rows(k_saved), feature_rows(v_saved)
        wqkv_t = jnp.transpose(w_qkv, (0, 2, 3, 1)).reshape(w_qkv.shape[0] * heads * dim, width)
        wo = w_proj.reshape(heads * dim, width)
        grad_x, grad_wfc1, grad_wfc2, dwqkv, dwo, db1, dbqkv, grad_vecs = backward(
            n_tp, scale, d_out, x_mid, z_saved, w_fc1, w_fc2, q_t, k_t, v_t, x_in, wqkv_t, wo,
            ln2_gain, ln2_bias, ln1_gain, ln1_bias)
        grad_x, grad_wfc1, grad_wfc2, dwqkv, dwo, db1, grad_bqkv, grad_vecs = place_results(
            (grad_x, grad_wfc1, grad_wfc2, dwqkv, dwo), db1, dbqkv, grad_vecs, (w_qkv.shape[0], heads, dim))
        grad_wqkv = jnp.transpose(dwqkv.reshape(-1, heads, dim, width), (0, 3, 1, 2))
        grad_wproj = dwo.reshape(heads, dim, width)
        return grad_x, grad_wqkv, grad_bqkv, grad_wproj, grad_wfc1, db1.reshape(-1), grad_wfc2, grad_vecs

    tok_spec = P('dp', 'tp', None)
    head_spec = P('dp', None, 'tp', None)
    in_specs = (tok_spec, tok_spec, tok_spec, head_spec, head_spec, head_spec, P('dp', None, 'tp'),
                P(None), P(None), P(None), P(None),
                P(None, None, 'tp', None), P('tp', None, None), P(None, 'tp'), P('tp', None))
    out_specs = (tok_spec, P('dp', None, 'tp', None), P('dp', 'tp', None), P(('dp', 'tp'), None, None),
                 P('dp', 'tp'), P(('dp', 'tp')), P(('dp', 'tp'), None), P('dp', None))
    return jax.shard_map(local_backward, mesh=mesh, in_specs=in_specs, out_specs=out_specs, check_vma=False)
```

```python
import functools

import jax
import jax.numpy as jnp
from jax import lax
from jax.experimental import pallas as pl
from jax.experimental.pallas import tpu as pltpu
from jax.sharding import PartitionSpec as P

LN_EPS = 1e-5
GELU_COEF = 0.044715
GELU_SCALE = 0.7978845608028654
LOG2E = 1.4426950408889634
MESH = pl.DeviceIdType.MESH
F32 = jnp.float32
BF16 = jnp.bfloat16
VMEM_LIMIT = 227 << 18

NN = (((1,), (0,)), ((), ()))
NT = (((1,), (1,)), ((), ()))
TN = (((0,), (0,)), ((), ()))

CORES = 2
BATCH = range(2)
HEADS = range(2)
RING = R_RIGHT, R_FAR, R_LEFT = 1, 2, 3
SLOT_P, SLOT_R, SLOT_F, SLOT_L, SLOT_END = 1, 2, 4, 6, 8
PARTNER, RIGHT, LEFT, FWD_R, FWD_L = range(5)
NEAR_R, NEAR_L, FAR_R, FAR_L, LAST_R, LAST_L = range(4, 10)
SUB = 8
LANES = 128
TK = 512
NC = 256
STEP = 64


def mm(a, b, dims):
    return lax.dot_general(a, b, dims, preferred_element_type=F32)


def loop(count, body):
    def run(i, carry):
        body(i)
        return carry
    lax.fori_loop(0, count, run, 0)


def fold8(v):
    return jnp.sum(v.reshape(v.shape[0] // SUB, SUB, v.shape[1]), axis=0)


def turn(v):
    return jnp.transpose(v.astype(F32)).astype(BF16)


def span(i, size):
    return pl.ds(pl.multiple_of(i * size, size), size)


def columns(width):
    return [pl.ds(n * NC, NC) for n in range(width // NC)]


def clear(*refs):
    for ref in refs:
        ref[...] = jnp.zeros_like(ref)


def ln_stats(rows):
    centered = rows - jnp.mean(rows, axis=-1, keepdims=True)
    inv_std = lax.rsqrt(jnp.mean(centered * centered, axis=-1, keepdims=True) + LN_EPS)
    return centered * inv_std, inv_std


def ln_bwd(grad, x_hat, inv_std, gain):
    grad_hat = grad * gain
    centered = grad_hat - jnp.mean(grad_hat, axis=-1, keepdims=True)
    return inv_std * (centered - x_hat * jnp.mean(grad_hat * x_hat, axis=-1, keepdims=True))


def normalize(src, dst, gain, bias, b):
    def body(i):
        rs = span(i, STEP)
        x_hat, _ = ln_stats(src[b, rs].astype(F32))
        dst[0, b, rs] = (x_hat * gain[...] + bias[...]).astype(BF16)

    loop(src.shape[1] // STEP, body)


def start_copies(pairs, sems):
    copies = [pltpu.make_async_copy(s, d, sems.at[i]) for i, (s, d) in enumerate(pairs)]
    for copy in copies:
        copy.start()
    return copies


class Place:
    def __init__(self, n_tp):
        self.chips = n_tp // CORES
        me = lax.axis_index('tp')
        self.x = me // CORES
        self.c = lax.rem(me, CORES)
        self.partner = self.block(0, 1)
        self.right, self.far, self.left = [self.block(r, 0) for r in RING]

    def block(self, r, p):
        return lax.rem(self.x + r, self.chips) * CORES + lax.rem(self.c + p, CORES)

    def enter(self, peers):
        barrier = pltpu.get_barrier_semaphore()
        for peer in peers:
            pl.semaphore_signal(barrier, inc=1, device_id={'tp': peer}, device_id_type=MESH)
        pl.semaphore_wait(barrier, len(peers))


def remote(src, dst, ssem, rsem, peer):
    return pltpu.make_async_remote_copy(src_ref=src, dst_ref=dst, send_sem=ssem, recv_sem=rsem,
                                        device_id={'tp': peer}, device_id_type=MESH)


class Gather:
    def __init__(self, place, own, buf, ssem, rsem):
        self.place, self.own, self.buf, self.ssem, self.rsem = place, own, buf, ssem, rsem
        half = buf.shape[-2] // 2
        self.lo, self.hi = pl.ds(0, half), pl.ds(half, half)

    def _own(self, kind, slot, b, peer):
        return remote(self.own.at[b], self.buf.at[slot, b], self.ssem.at[kind, b], self.rsem.at[slot, b], peer)

    def to_partner(self, b):
        return self._own(PARTNER, SLOT_P, b, self.place.partner)

    def to_right(self, b):
        return self._own(RIGHT, SLOT_L, b, self.place.right)

    def to_left(self, b):
        return self._own(LEFT, SLOT_R, b, self.place.left)

    def fwd_right(self, b):
        return remote(self.buf.at[SLOT_L, b, self.lo], self.buf.at[SLOT_F, b, self.lo],
                      self.ssem.at[FWD_R, b], self.rsem.at[SLOT_F, b], self.place.right)

    def fwd_left(self, b):
        return remote(self.buf.at[SLOT_R, b, self.hi], self.buf.at[SLOT_F, b, self.hi],
                      self.ssem.at[FWD_L, b], self.rsem.at[SLOT_END, b], self.place.left)

    def share(self, r, b):
        slot = CORES * r
        return remote(self.buf.at[slot, b], self.buf.at[slot + 1, b], self.ssem.at[FWD_L + r, b], self.rsem.at[slot + 1, b],
                      self.place.partner)

    def start_own(self, b):
        self.to_right(b).start()
        self.to_left(b).start()
        self.to_partner(b).start()

    def relay(self, b):
        self.to_right(b).wait_recv()
        self.fwd_right(b).start()
        self.to_left(b).wait_recv()
        self.fwd_left(b).start()
        self.share(R_LEFT, b).start()
        self.share(R_RIGHT, b).start()

    def relay_far(self, b):
        self.fwd_right(b).wait_recv()
        self.fwd_left(b).wait_recv()
        self.share(R_FAR, b).start()

    def wait_shared(self, r, b):
        self.share(r, b).wait_recv()

    def wait_partner(self, b):
        self.to_partner(b).wait_recv()

    def drain_own(self, b):
        for copy in (self.to_partner, self.to_right, self.to_left):
            copy(b).wait_send()

    def drain_near(self, b):
        for copy in (self.fwd_right(b), self.fwd_left(b), self.share(R_RIGHT, b), self.share(R_LEFT, b)):
            copy.wait_send()

    def drain_far(self, b):
        self.share(R_FAR, b).wait_send()

    def drain(self, b):
        self.drain_own(b)
        self.drain_near(b)
        self.drain_far(b)


class Scatter:
    def __init__(self, place, p_out, p_in, sums, fin, transit, ssem, rsem):
        self.place = place
        self.p_out, self.p_in, self.sums, self.fin, self.transit = p_out, p_in, sums, fin, transit
        self.ssem, self.rsem = ssem, rsem
        half = sums.shape[-2] // 2
        self.lo, self.hi = pl.ds(0, half), pl.ds(half, half)

    def to_partner(self, r, b):
        return remote(self.p_out.at[r, b], self.p_in.at[r, b], self.ssem.at[r, b], self.rsem.at[r, b], self.place.partner)

    def _hop(self, kind, src, dst, b, peer):
        return remote(src, dst, self.ssem.at[kind, b], self.rsem.at[kind, b], peer)

    def near_right(self, b):
        return self._hop(NEAR_R, self.sums.at[0, b, self.hi], self.fin.at[0, b, self.hi], b, self.place.right)

    def near_left(self, b):
        return self._hop(NEAR_L, self.sums.at[2, b, self.lo], self.fin.at[1, b, self.lo], b, self.place.left)

    def far_right(self, b):
        return self._hop(FAR_R, self.sums.at[1, b, self.lo], self.transit.at[0, b], b, self.place.right)

    def far_left(self, b):
        return self._hop(FAR_L, self.sums.at[1, b, self.hi], self.transit.at[1, b], b, self.place.left)

    def last_right(self, b):
        return self._hop(LAST_R, self.sums.at[0, b, self.lo], self.fin.at[0, b, self.lo], b, self.place.right)

    def last_left(self, b):
        return self._hop(LAST_L, self.sums.at[2, b, self.hi], self.fin.at[1, b, self.hi], b, self.place.left)

    def send_near(self, b):
        self.near_right(b).start()
        self.near_left(b).start()

    def send_far(self, b):
        self.far_right(b).start()
        self.far_left(b).start()

    def send_last(self, b):
        for arrived, slot, lane, rows, onward in ((self.far_right, 0, 0, self.lo, self.last_right),
                                                  (self.far_left, 2, 1, self.hi, self.last_left)):
            arrived(b).wait_recv()
            self.sums[slot, b, rows] = (self.sums[slot, b, rows].astype(F32) + self.transit[lane, b].astype(F32)).astype(BF16)
            onward(b).start()

    def wait_final(self, b):
        for copy in (self.near_right, self.near_left, self.last_right, self.last_left):
            copy(b).wait_recv()

    def total(self, own, b, rs):
        return own[b, rs] + self.fin[0, b, rs].astype(F32) + self.fin[1, b, rs].astype(F32)

    def finish(self):
        for b in BATCH:
            for r in (0, *RING):
                self.to_partner(r, b).wait_send()
            for copy in (self.near_right, self.near_left, self.far_right, self.far_left, self.last_right, self.last_left):
                copy(b).wait_send()


def scatter_scratch(rows, width):
    def buf(*lead):
        return pltpu.VMEM((*lead, len(BATCH), rows, width), BF16)
    return [buf(4), buf(4), buf(3), buf(2), pltpu.VMEM((2, len(BATCH), rows // 2, width), BF16)]


def copy_sems(*counts):
    return [pltpu.SemaphoreType.DMA((count, len(BATCH))) for count in counts]


def first_head(shape):
    return lax.broadcasted_iota(jnp.int32, shape, 1) < shape[1] // len(HEADS)


def split_heads(v):
    first, zero = first_head(v.shape), jnp.zeros_like(v)
    return [jnp.where(first, v, zero), jnp.where(first, zero, v)]


def visible(blk, j, rows):
    row_id = blk * rows + lax.broadcasted_iota(jnp.int32, (rows, TK), 0)
    return row_id >= j * TK + lax.broadcasted_iota(jnp.int32, (rows, TK), 1)


def attn_fwd_block(b, blk, q_t, k_t, v_t, ctx_t, ctx, lse, s_buf, m_buf, scale):
    rows = ctx.shape[2]
    qs = span(blk, rows)
    last = blk // (TK // rows)
    q_h = split_heads(turn(q_t[b, :, qs]))

    def fold(f, v):
        parts = [v[:, i:i + LANES] for i in range(0, TK, LANES)]
        return functools.reduce(f, parts)

    def score(j, masked=False):
        kk = k_t[b, :, span(j, TK)]
        for h in HEADS:
            s = mm(q_h[h], kk, NN) * scale
            if masked:
                s = jnp.where(visible(blk, j, rows), s, -1e30)
            s_buf[h, :, span(j, TK)] = s
            top = fold(jnp.maximum, s)
            m_buf[h] = top if masked else jnp.maximum(m_buf[h], top)

    score(last, True)
    loop(last, score)
    m_col = [jnp.max(m_buf[h], axis=-1, keepdims=True) for h in HEADS]
    clear(m_buf)

    def total(j):
        for h in HEADS:
            m_buf[h] += fold(jnp.add, jnp.exp2(s_buf[h, :, span(j, TK)] - m_col[h]))

    loop(last + 1, total)
    l_col = [m_col[h] + jnp.log2(jnp.sum(m_buf[h], axis=-1, keepdims=True)) for h in HEADS]
    clear(m_buf)

    def weigh(j):
        vv = v_t[b, :, span(j, TK)]
        for h in HEADS:
            m_buf[h] += mm(jnp.exp2(s_buf[h, :, span(j, TK)] - l_col[h]).astype(BF16), vv, NT)

    loop(last + 1, weigh)
    first = first_head(m_buf.shape[1:])
    out = jnp.where(first, m_buf[0], m_buf[1])
    ctx[b, blk] = out
    lse_t = jnp.transpose(jnp.where(first, *l_col))
    for h in HEADS:
        top = h * (LANES // len(HEADS))
        lse[b, blk, h:h + 1] = lse_t[top:top + 1]
    ctx_t[b, :, qs] = turn(out)


def backward_kernel(n_tp, scale, dy_hbm, xm_hbm, z_hbm, w1_hbm, w2_hbm, q_hbm, k_hbm, v_hbm, xi_hbm, wqkv_hbm, wo_hbm,
                    gain2_ref, bias2_ref, gain1_ref, bias1_ref,
                    xi, dw1, dw2, dwqkv, dwo, db1_ref, dbqkv_ref, vecs_ref,
                    tok, hb, p_out, p_in, sums, fin, transit,
                    z, w1, w2, own, xm, db1, q_t, k_t, v_t, ctx_t, ctx, lse, acc, head_acc,
                    wqkv, wo, dqkv, vacc, vsend, vrecv,
                    dy_ss, dy_rs, h2_ss, h2_rs, dx_ss, dx_rs, h1_ss, h1_rs, rs2_ss, rs2_rs, rs1_ss, rs1_rs,
                    lsem, v_ss, v_rs, credit):
    place = Place(n_tp)
    rows, width = dy_hbm.shape[1:]
    units = w2.shape[0]
    blocks = ctx.shape[1]
    neighbours = (place.partner, place.right, place.left)
    place.enter((*neighbours, place.far))
    dyg = Gather(place, dy_hbm, tok, dy_ss, dy_rs)
    mg = Gather(place, tok.at[0], tok, dx_ss, dx_rs)
    h2g = Gather(place, hb.at[0], hb, h2_ss, h2_rs)
    h1g = Gather(place, hb.at[0], hb, h1_ss, h1_rs)
    sc2 = Scatter(place, p_out, p_in, sums, fin, transit, rs2_ss, rs2_rs)
    sc1 = Scatter(place, p_out, p_in, sums, fin, transit, rs1_ss, rs1_rs)
    for b in BATCH:
        dyg.start_own(b)
    loads = start_copies(((xm_hbm, xm), (dy_hbm, tok.at[0]), (w2_hbm, w2), (z_hbm, z), (w1_hbm, w1),
                          (q_hbm, q_t), (k_hbm, k_t), (v_hbm, v_t), (wo_hbm, wo), (wqkv_hbm, wqkv), (xi_hbm, xi)), lsem)
    clear(dw1, dw2, db1, vacc, vsend, dwqkv, dwo, lse)
    loads[0].wait()
    loop(2, functools.partial(normalize, xm, hb, gain2_ref, bias2_ref))
    for load in loads[1:]:
        load.wait()
    exp_scale = scale * LOG2E
    dim = LANES // len(HEADS)

    def recall(lo, count):
        def body(i):
            i = lo + i
            attn_fwd_block(i // blocks, lax.rem(i, blocks), q_t, k_t, v_t, ctx_t, ctx, lse, acc, head_acc, exp_scale)
        loop(count, body)

    def pre_piece(r, p, b):
        dy, blk = tok[CORES * r + p, b], place.block(r, p)
        for fs in columns(units):
            act = mm(dy, w2[fs, :], NT)
            zf = z[b, blk, :, fs].astype(F32)
            t = jnp.tanh(GELU_SCALE * (zf + GELU_COEF * zf * zf * zf))
            half_t = 0.5 * (1.0 + t)
            slope = half_t + 0.5 * zf * (1.0 - t * t) * GELU_SCALE * (1.0 + 3.0 * GELU_COEF * zf * zf)
            u = (zf * half_t).astype(BF16)
            dzv = (act * slope).astype(BF16)
            z[b, blk, :, fs] = dzv
            db1[:, fs] += fold8(dzv.astype(F32))
            dw2[fs, :] += mm(u, dy, TN)
        return z[b, blk]

    def pair(r, b, put):
        dz = pre_piece(r, 1, b)
        for ns in columns(width):
            p_out[r, b, :, ns] = mm(dz, w1[ns, :], NT).astype(BF16)
        sc2.to_partner(r, b).start()
        dz = pre_piece(r, 0, b)
        sc2.to_partner(r, b).wait_recv()
        for ns in columns(width):
            put(ns, mm(dz, w1[ns, :], NT) + p_in[r, b, :, ns].astype(F32))

    def pair_out(r, b):
        dyg.wait_shared(r, b)

        def put(ns, v):
            sums[r - 1, b, :, ns] = v.astype(BF16)
        pair(r, b, put)

    def own_body(b):
        dyg.wait_partner(b)

        def put(ns, v):
            own[b, :, ns] = v
        pair(0, b, put)

    def near_body(b):
        dyg.relay(b)
        loop(2, lambda i: pair_out(R_RIGHT + 2 * i, b))
        sc2.send_near(b)
        recall(2 * b, 2)

    def far_body(b):
        dyg.relay_far(b)
        pair_out(R_FAR, b)
        dyg.drain_far(b)
        sc2.send_far(b)
        h2g.start_own(b)

    def dw1_pair(r, b):
        def body(p):
            dz = z[b, place.block(r, p)]
            for ns in columns(width):
                dw1[ns, :] += mm(hb[CORES * r + p, b, :, ns], dz, TN)
        loop(CORES, body)

    def dw1_own(b):
        h2g.wait_partner(b)
        dw1_pair(0, b)

    def dw1_near(b):
        def body(i):
            r = R_RIGHT + 2 * i
            h2g.wait_shared(r, b)
            dw1_pair(r, b)
        loop(2, body)

    def dw1_far(b):
        h2g.relay_far(b)
        h2g.wait_shared(R_FAR, b)
        dw1_pair(R_FAR, b)
        h2g.drain(b)
        for peer in neighbours:
            pl.semaphore_signal(credit.at[b], inc=1, device_id={'tp': peer}, device_id_type=MESH)
        normalize(xi, hb, gain1_ref, bias1_ref, b)

    def start_h1(b):
        pl.semaphore_wait(credit.at[b], len(neighbours))
        h1g.start_own(b)

    def back2(b):
        sc2.wait_final(b)

        def body(i):
            rs = span(i, STEP)
            grad = sc2.total(own, b, rs)
            x_hat, inv_std = ln_stats(xm[b, rs].astype(F32))
            dyf = tok[0, b, rs].astype(F32)
            dx1 = (dyf + ln_bwd(grad, x_hat, inv_std, gain2_ref[...])).astype(BF16)
            tok[0, b, rs] = dx1
            for k, v in enumerate((grad * x_hat, grad, dx1.astype(F32), dyf)):
                vacc[2 + k] += fold8(v)
        loop(rows // STEP, body)
        mg.start_own(b)

    def last2(b):
        dyg.drain_near(b)
        sc2.send_last(b)

    def attend(r, p, b):
        mid, blk = tok[CORES * r + p, b], place.block(r, p)
        qs = span(blk, rows)
        dwo[...] += mm(ctx_t[b, :, qs], mid, NN)
        dctx = mm(mid, wo[...], NT).astype(BF16)
        dctx_t = turn(dctx)
        qt = q_t[b, :, qs]
        q_h, d_h = split_heads(turn(qt)), split_heads(dctx)
        delta = [jnp.sum(v, axis=-1, keepdims=True) for v in split_heads(dctx.astype(F32) * ctx[b, blk])]
        lse_v = jnp.transpose(lse[b, blk])
        l_col = [lse_v[:, h:h + 1] for h in HEADS]
        last = blk // (TK // rows)
        clear(head_acc)

        def tile(j, masked=False):
            ks = span(j, TK)
            kk, vv = k_t[b, :, ks], v_t[b, :, ks]
            for h in HEADS:
                hs = pl.ds(pl.multiple_of(b * LANES + h * dim, dim), dim)
                top = slice(h * dim, (h + 1) * dim)
                prob = jnp.exp2(mm(q_h[h], kk, NN) * exp_scale - l_col[h])
                if masked:
                    prob = jnp.where(visible(blk, j, rows), prob, 0.0)
                ds = (prob * (mm(d_h[h], vv, NN) - delta[h])).astype(BF16)
                head_acc[h] += mm(ds, kk, NT)
                acc[0, hs, ks] += mm(qt[top], ds, NN)
                acc[1, hs, ks] += mm(dctx_t[top], prob.astype(BF16), NN)

        tile(last, True)
        loop(last, tile)
        dq = jnp.where(first_head(head_acc.shape[1:]), head_acc[0], head_acc[1]) * scale
        dqkv[b, :LANES, qs] = turn(dq)

    def attend_own(i):
        b, p = i // CORES, lax.rem(i, CORES)

        @pl.when(p == 0)
        def _():
            mg.wait_partner(b)
        attend(0, p, b)

    def attend_near(b):
        for r in (R_RIGHT, R_LEFT):
            mg.wait_shared(r, b)

        def body(i):
            @pl.when((i == 2 * CORES - 1) & (b == 0))
            def _():
                mg.relay(1)
                for k in BATCH:
                    start_h1(k)
            attend(R_RIGHT + 2 * (i // CORES), lax.rem(i, CORES), b)
        loop(2 * CORES, body)

    def partial_rows(r, p, b):
        return turn(dqkv[b, :, span(place.block(r, p), rows)])

    def reduce_out(r, b):
        lhs = partial_rows(r, 0, b)
        sc1.to_partner(r, b).wait_recv()
        for ns in columns(width):
            sums[r - 1, b, :, ns] = (mm(lhs, wqkv[:, ns], NN) + p_in[r, b, :, ns].astype(F32)).astype(BF16)

    def attend_far(b):
        @pl.when(b == 0)
        def _():
            mg.relay_far(0)
        mg.wait_shared(R_FAR, b)
        loop(CORES, lambda p: attend(R_FAR, p, b))
        mine = span(b, LANES)
        dqkv[b, LANES:2 * LANES] = (acc[0, mine] * scale).astype(BF16)
        dqkv[b, 2 * LANES:] = acc[1, mine].astype(BF16)

        def to_partner(i):
            r = lax.rem(R_FAR + i, place.chips)
            lhs = partial_rows(r, 1, b)
            for ns in columns(width):
                p_out[r, b, :, ns] = mm(lhs, wqkv[:, ns], NN).astype(BF16)
            sc1.to_partner(r, b).start()

        loop(place.chips, to_partner)
        reduce_out(R_FAR, b)
        sc1.send_far(b)
        loop(2, lambda i: reduce_out(R_RIGHT + 2 * i, b))
        sc1.send_near(b)
        lhs = partial_rows(0, 0, b)
        sc1.to_partner(0, b).wait_recv()
        for ns in columns(width):
            own[b, :, ns] = mm(lhs, wqkv[:, ns], NN) + p_in[0, b, :, ns].astype(F32)

    def dw_pair(r, b):
        def body(p):
            part = dqkv[b, :, span(place.block(r, p), rows)]
            for ns in columns(width):
                dwqkv[:, ns] += mm(part, hb[CORES * r + p, b, :, ns], NN)
        loop(CORES, body)

    def dw_own(b):
        h1g.wait_partner(b)
        dw_pair(0, b)

    def dw_near(b):
        def body(i):
            r = R_RIGHT + 2 * i
            h1g.wait_shared(r, b)
            dw_pair(r, b)
        loop(2, body)

    def dw_far(b):
        h1g.relay_far(b)
        h1g.wait_shared(R_FAR, b)
        dw_pair(R_FAR, b)

    def back1(b):
        sc1.wait_final(b)

        def body(i):
            rs = span(i, STEP)
            grad = sc1.total(own, b, rs)
            x_hat, inv_std = ln_stats(xi[b, rs].astype(F32))
            dx = (tok[0, b, rs].astype(F32) + ln_bwd(grad, x_hat, inv_std, gain1_ref[...])).astype(BF16)
            xi[b, rs] = dx
            for k, v in enumerate((grad * x_hat, grad)):
                vacc[k] += fold8(v)
        loop(rows // STEP, body)

    loop(2, own_body)
    loop(2, near_body)
    loop(2, far_body)
    tail = 3
    recall(4, 2 * blocks - 4 - tail)
    loop(2, last2)
    recall(2 * blocks - tail, tail)
    clear(acc)
    h2g.relay(0)
    loop(2, dw1_own)
    h2g.relay(1)
    loop(2, dw1_near)
    loop(2, back2)
    sc2.finish()
    loop(len(BATCH) * CORES, attend_own)
    loop(2, dw1_far)
    db1_ref[...] = jnp.sum(db1[...], axis=0, keepdims=True)
    mg.relay(0)

    def batch(b):
        @pl.when(b == 1)
        def _():
            mg.relay_far(1)
        attend_near(b)
        attend_far(b)

    loop(2, batch)
    sc1.send_last(0)
    h1g.relay(0)
    loop(2, dw_own)
    ones = jnp.ones((SUB, dqkv.shape[2]), BF16)
    dbqkv = (mm(ones, dqkv[0], NT) + mm(ones, dqkv[1], NT))[:1]
    for i in range(dbqkv_ref.shape[0]):
        for h in HEADS:
            start = i * LANES + h * dim
            dbqkv_ref[i, h:h + 1] = dbqkv[:, start:start + dim]
    sc1.send_last(1)
    h1g.relay(1)
    loop(2, dw_near)
    loop(2, back1)
    for k in range(vacc.shape[0]):
        vsend[k:k + 1] = jnp.sum(vacc[k], axis=0, keepdims=True)
    swap = remote(vsend, vrecv, v_ss.at[0], v_rs.at[n_tp], place.partner)
    swap.start()
    swap.wait_recv()

    def vring(chip):
        return acc.at[0, span(chip, SUB), pl.ds(0, width)]

    vring(place.x)[...] = vsend[...] + vrecv[...]
    ring = [remote(vring(place.x), vring(place.x), v_ss.at[r], v_rs.at[place.x], peer)
            for r, peer in zip(RING, (place.right, place.far, place.left))]
    for copy in ring:
        copy.start()
    loop(2, dw_far)
    for r in RING:
        other = lax.rem(place.x + r, place.chips)
        remote(vring(other), vring(other), v_ss.at[r], v_rs.at[other], place.right).wait_recv()
    vecs_ref[...] = functools.reduce(jnp.add, [vring(k)[...] for k in range(place.chips)])[:vecs_ref.shape[0]]
    swap.wait_send()
    for copy in ring:
        copy.wait_send()
    for b in BATCH:
        dyg.drain_own(b)
        mg.drain(b)
        h1g.drain(b)
    sc1.finish()


def backward(n_tp, scale, d_out, x_mid, z, w1, w2, q_t, k_t, v_t, x_in, wqkv_t, wo, gain2, bias2, gain1, bias1):
    batch, rows, width = d_out.shape
    units = w2.shape[0]
    seq = q_t.shape[2]
    blocks = seq // rows
    qkv_rows = wqkv_t.shape[0]
    any_spec = pl.BlockSpec(memory_space=pl.ANY)
    vm = pl.BlockSpec(memory_space=pltpu.VMEM)
    slots = pltpu.VMEM((SLOT_END, batch, rows, width), BF16)
    row = pltpu.VMEM((SUB, width), F32)

    return pl.pallas_call(
        functools.partial(backward_kernel, n_tp, scale),
        name='layer_backward',
        out_shape=(pltpu.VMEM((batch, rows, width), BF16), pltpu.VMEM((width, units), F32), pltpu.VMEM((units, width), F32),
                   pltpu.VMEM((qkv_rows, width), F32), pltpu.VMEM((LANES, width), F32),
                   pltpu.VMEM((1, units), F32), pltpu.VMEM((qkv_rows // LANES, len(HEADS), LANES // len(HEADS)), F32), pltpu.VMEM((6, width), F32)),
        in_specs=[any_spec] * 11 + [vm] * 4,
        out_specs=(vm,) * 8,
        scratch_shapes=[
            slots, slots, *scatter_scratch(rows, width),
            pltpu.VMEM((batch, blocks, rows, units), BF16),
            pltpu.VMEM((width, units), BF16), pltpu.VMEM((units, width), BF16),
            pltpu.VMEM((batch, rows, width), F32), pltpu.VMEM((batch, rows, width), BF16),
            pltpu.VMEM((SUB, units), F32), *[pltpu.VMEM((batch, LANES, seq), BF16)] * 4,
            pltpu.VMEM((batch, blocks, rows, LANES), F32), pltpu.VMEM((batch, blocks, SUB, rows), F32),
            pltpu.VMEM((len(HEADS), rows, seq), F32), pltpu.VMEM((len(HEADS), rows, LANES), F32),
            pltpu.VMEM((qkv_rows, width), BF16), pltpu.VMEM((LANES, width), BF16), pltpu.VMEM((batch, qkv_rows, seq), BF16),
            pltpu.VMEM((6, SUB, width), F32), row, row,
            *copy_sems(*[SLOT_END, SLOT_END + 1] * 4, *[10] * 4),
            pltpu.SemaphoreType.DMA((11,)), pltpu.SemaphoreType.DMA((4,)), pltpu.SemaphoreType.DMA((n_tp + 1,)),
            pltpu.SemaphoreType.REGULAR((batch,)),
        ],
        compiler_params=pltpu.CompilerParams(collective_id=1, has_side_effects=True, vmem_limit_bytes=VMEM_LIMIT),
    )(d_out, x_mid, z.reshape(batch, blocks, rows, units), w1, w2, q_t, k_t, v_t, x_in, wqkv_t, wo,
      *[v.reshape(1, width) for v in (gain2, bias2, gain1, bias1)])


def place_results(results):
    count = len(results)

    def kernel(*refs):
        for move in start_copies(zip(refs[:count], refs[count:-1]), refs[-1]):
            move.wait()

    return pl.pallas_call(
        kernel,
        name='place_results',
        out_shape=[jax.ShapeDtypeStruct(v.shape, v.dtype) for v in results],
        in_specs=[pl.BlockSpec(memory_space=pltpu.VMEM)] * count,
        out_specs=[pl.BlockSpec(memory_space=pl.ANY)] * count,
        scratch_shapes=[pltpu.SemaphoreType.DMA((count,))],
        compiler_params=pltpu.CompilerParams(vmem_limit_bytes=8 << 20),
    )(*[pltpu.with_memory_space_constraint(v, pltpu.VMEM) for v in results])


def solution(mesh):
    n_tp = mesh.shape['tp']

    def local_backward(x_in, x_mid, d_out, q_saved, k_saved, v_saved, z_saved, ln1_gain, ln1_bias, ln2_gain, ln2_bias, w_qkv, w_proj, w_fc1, w_fc2):
        batch, seq, heads, dim = q_saved.shape
        width = x_in.shape[-1]
        scale = dim ** -0.5

        def feature_rows(a):
            return jnp.transpose(a, (0, 2, 3, 1)).reshape(batch, heads * dim, seq)

        q_t, k_t, v_t = feature_rows(q_saved), feature_rows(k_saved), feature_rows(v_saved)
        wqkv_t = jnp.transpose(w_qkv, (0, 2, 3, 1)).reshape(w_qkv.shape[0] * heads * dim, width)
        wo = w_proj.reshape(heads * dim, width)
        grad_x, grad_wfc1, grad_wfc2, dwqkv, dwo, db1, grad_bqkv, grad_vecs = place_results(backward(
            n_tp, scale, d_out, x_mid, z_saved, w_fc1, w_fc2, q_t, k_t, v_t, x_in, wqkv_t, wo,
            ln2_gain, ln2_bias, ln1_gain, ln1_bias))
        grad_wqkv = jnp.transpose(dwqkv.reshape(-1, heads, dim, width), (0, 3, 1, 2))
        grad_wproj = dwo.reshape(heads, dim, width)
        return grad_x, grad_wqkv, grad_bqkv, grad_wproj, grad_wfc1, db1.reshape(-1), grad_wfc2, grad_vecs

    tok_spec = P('dp', 'tp', None)
    head_spec = P('dp', None, 'tp', None)
    in_specs = (tok_spec, tok_spec, tok_spec, head_spec, head_spec, head_spec, P('dp', None, 'tp'),
                P(None), P(None), P(None), P(None),
                P(None, None, 'tp', None), P('tp', None, None), P(None, 'tp'), P('tp', None))
    out_specs = (tok_spec, P('dp', None, 'tp', None), P('dp', 'tp', None), P(('dp', 'tp'), None, None),
                 P('dp', 'tp'), P(('dp', 'tp')), P(('dp', 'tp'), None), P('dp', None))
    return jax.shard_map(local_backward, mesh=mesh, in_specs=in_specs, out_specs=out_specs, check_vma=False)
```
